32 devices in a mesh: dom: 16 (over z, y, core), st: 2 (over x).
Axes of the slice: x: 2, y: 2, z: 4, core: 2. Of those that a mesh axis runs over, the one named last changes fastest.
Arguments:
- start_states: bfloat16 [512, 57344], P('st', 'dom'), may hold values from -6 to 6
- stiffness: bfloat16 [512, 512], replicated, may hold values from -1 to 3
- cell_scale: float32 [128], P('dom'), may hold values from 0.5 to 2
- potential: float32 [57344], P('dom'), may hold values from -2 to 2
- connectivity: int32 [128, 512], P('dom'), may hold values from 0 to 3479, as said below
- shared_nodes: int32 [16, 2, 435], P('dom'), may hold values from 0 to 3479, as said below
- filter_bounds: float32 [2], replicated, may hold values from 3 to 60, as said below
Outputs:
- new_states: bfloat16 [512, 57344], P('st', 'dom')
The draws below stay inside these ranges and needn't reach their ends.
Inputs may be any that keep to these rules, and one draw needn't show every extreme that they name: `connectivity`: for each domain, its cells' entries name every one of its 3480 local nodes; nodes of a domain are numbered in a drawn order; cells of a domain share nodes as hexahedral elements of order 7 do. shared_nodes[d, 1] and shared_nodes[d + 1, 0] list the same mesh nodes in the same order; within one domain the two lists are distinct nodes and disjoint. filter_bounds[0] < filter_bounds[1].
All inputs are finite; a program needn't handle non-finite values.
Results may differ from the reference program's by a relative error of at most 0.0049.
The reference program's roundings to bfloat16 on the way count: a program that leaves them out, or rounds other values in their place, can miss the bound.
Values may be sent and summed in bfloat16 or wider, within the bound.
No kernel may reach another device: no remote copies, remote signals or barrier semaphores. Data moves between devices by JAX's collectives and lax.ppermute only.
A program may use at most 64 MiB of HBM per device.

```python
import math
import jax
import jax.numpy as jnp
from jax import lax

ORDER = 7
NPC = 512
CB = 4
CC = 1
NS = 512
DEGREE = 3
NS_ITERS = 3
DOMS = 16
CELLS = 8
LN = 3480
LNP = 3584
SH = 435


def node_tables(key):
    base = jax.random.fold_in(key, 4242)
    per_edge = ORDER + 1
    node_across = CB * ORDER + 1
    node_depth = CC * ORDER + 1
    cell_ids = jnp.arange(CELLS)
    dof_ids = jnp.arange(NPC)
    cell_first = cell_ids // (CB * CC)
    cell_second = cell_ids // CC % CB
    cell_third = cell_ids % CC
    dof_first = dof_ids // (per_edge * per_edge)
    dof_second = dof_ids // per_edge % per_edge
    dof_third = dof_ids % per_edge
    coord_first = cell_first[:, None] * ORDER + dof_first[None, :]
    coord_second = cell_second[:, None] * ORDER + dof_second[None, :]
    coord_third = cell_third[:, None] * ORDER + dof_third[None, :]
    structured = (coord_first * node_across + coord_second) * node_depth + coord_third
    face_ids = jnp.arange(SH)
    face_row = face_ids // node_across
    face_col = face_ids % node_across
    left_face = (face_row * node_across + face_col) * node_depth
    right_face = left_face + node_depth - 1
    domain_keys = jax.random.split(base, DOMS)

    def number_domain(domain_key):
        shuffle = jax.random.permutation(domain_key, LN).astype(jnp.int32)
        return (shuffle[structured], jnp.stack([shuffle[left_face], shuffle[right_face]]))
    return jax.vmap(number_domain)(domain_keys)


def draw_connectivity(key, part):
    tables = node_tables(key)
    return tables[0].reshape(DOMS * CELLS, NPC).astype(jnp.int32)


def draw_shared_nodes(key, part):
    tables = node_tables(key)
    return tables[1].astype(jnp.int32)


def draw_stiffness(key, part):
    inner_key = jax.random.fold_in(key, 77)
    base_mat = jax.random.normal(inner_key, (NPC, NPC), jnp.float32)
    matrix = jnp.dot(base_mat, base_mat.T, precision=jax.lax.Precision.HIGHEST) / NPC
    matrix = matrix + 0.25 * jnp.eye(NPC, dtype=jnp.float32)
    return matrix.astype(jnp.bfloat16)


def draw_filter_bounds(key, part):
    first_key, second_key = jax.random.split(jax.random.fold_in(key, 91))
    bottom = jax.random.uniform(first_key, (), jnp.float32, 4.0, 8.0)
    ceiling = jax.random.uniform(second_key, (), jnp.float32, 30.0, 50.0)
    return jnp.stack([bottom, ceiling]).astype(jnp.float32)


def block_scale(key, extent, shards, low, top_value):
    def one(axis_at, shards_of):
        heights = jax.random.uniform(jax.random.fold_in(jax.random.fold_in(key, 6), axis_at), (shards_of,), jnp.float32, low / len(shards), top_value / len(shards))
        return jnp.repeat(jnp.exp(heights), extent[axis_at] // shards_of).reshape((-1,) + (1,) * (len(extent) - axis_at - 1))

    level = one(*shards[0])
    for cut in shards[1:]:
        level = level * one(*cut)
    return level


def noise(stream_key, shape, spread, most, cuts=(), kind=jnp.bfloat16):
    level = block_scale(stream_key, shape, cuts, -0.22, 0.18) if cuts else 1.0
    result = jax.random.normal(stream_key, shape, jnp.float32) * spread * level
    return jnp.minimum(jnp.maximum(result, -most), most).astype(kind)


def setup_inputs(seed: int = 0) -> dict:
    keys = jax.random.split(jax.random.key(seed), 8)
    start_states = noise(keys[0], (NS, DOMS * LNP), 1.0, 6.0, ((0, 2), (1, 16)))
    stiffness = draw_stiffness(jax.random.fold_in(keys[7], 71), 0)
    cell_scale = jnp.clip(jnp.exp(math.log(2.0) - 1.3862944 * jax.random.uniform(keys[2], (DOMS * CELLS,), jnp.float32) ** block_scale(keys[2], (DOMS * CELLS,), ((0, 16),), -0.2, 0.2)), 0.5, 2.0)
    potential = jnp.clip(jax.random.uniform(keys[3], (DOMS * LNP,), jnp.float32, -2.0, 2.0) * block_scale(keys[3], (DOMS * LNP,), ((0, 16),), -0.4, 0.0), -2.0, 2.0)
    connectivity = draw_connectivity(jax.random.fold_in(keys[7], 71), 0)
    shared_nodes = draw_shared_nodes(jax.random.fold_in(keys[7], 71), 0)
    filter_bounds = draw_filter_bounds(jax.random.fold_in(keys[7], 71), 0)
    return {"start_states": start_states, "stiffness": stiffness, "cell_scale": cell_scale, "potential": potential, "connectivity": connectivity, "shared_nodes": shared_nodes, "filter_bounds": filter_bounds}


def inverse_root(gram):
    frobenius = jnp.sqrt(jnp.sum(gram * gram) + 1e-06)
    iterate = gram / frobenius
    identity = jnp.eye(gram.shape[0], dtype=jnp.float32)
    inverse = identity
    for sweep in range(NS_ITERS):
        factor = 1.5 * identity - 0.5 * jnp.dot(inverse, iterate, precision=lax.Precision.HIGHEST)
        iterate = jnp.dot(iterate, factor, precision=lax.Precision.HIGHEST)
        inverse = jnp.dot(factor, inverse, precision=lax.Precision.HIGHEST)
    return (inverse / jnp.sqrt(frobenius)).astype(jnp.bfloat16)

def reference(start_states, stiffness, cell_scale, potential, connectivity, shared_nodes, filter_bounds):
    states = start_states.reshape(NS, DOMS, LNP).transpose(1, 0, 2)
    node_ids = jnp.arange(LNP)
    inside = (node_ids < LN).astype(jnp.bfloat16)
    states = states * inside[None, None, :]
    links_all = connectivity.reshape(DOMS, CELLS, NPC)
    scales = cell_scale.reshape(DOMS, CELLS)
    pot_all = potential.reshape(DOMS, LNP)
    stiff_wide = stiffness.astype(jnp.float32)
    left_ids = shared_nodes[:, 0]
    right_ids = shared_nodes[:, 1]

    def domain_term(items):
        block, links, scaled, pot_row = items
        values = block[:, links].astype(jnp.float32)
        products = jnp.einsum('scn,nm->scm', values, stiff_wide) * scaled[None, :, None]
        total = jnp.zeros(block.shape, jnp.float32).at[:, links.reshape(-1)].add(products.reshape(block.shape[0], -1))
        return total + pot_row[None, :] * block.astype(jnp.float32)

    def operate_all(field):
        terms = lax.map(domain_term, (field, links_all, scales, pot_all))
        right_vals = jax.vmap(lambda term, ids: term[:, ids])(terms, right_ids)
        left_vals = jax.vmap(lambda term, ids: term[:, ids])(terms, left_ids)
        zero_face = jnp.zeros_like(right_vals[:1])
        from_below = jnp.concatenate([zero_face, right_vals[:-1]], axis=0)
        from_above = jnp.concatenate([left_vals[1:], zero_face], axis=0)

        def combine(term, lower_ids, upper_ids, below, above):
            return term.at[:, lower_ids].add(below).at[:, upper_ids].add(above)
        return jax.vmap(combine)(terms, left_ids, right_ids, from_below, from_above)
    center = (filter_bounds[1] + filter_bounds[0]) / 2.0
    half_width = (filter_bounds[1] - filter_bounds[0]) / 2.0
    previous = states
    current = ((operate_all(states) - center * states.astype(jnp.float32)) / half_width).astype(jnp.bfloat16)
    for degree_step in range(DEGREE - 1):
        following = 2.0 * (operate_all(current) - center * current.astype(jnp.float32)) / half_width - previous.astype(jnp.float32)
        previous, current = (current, following.astype(jnp.bfloat16))
    domain_ids = jnp.arange(DOMS)

    def owned_mask(domain, lower_ids):
        keep = jnp.where(domain > 0, 0.0, 1.0).astype(jnp.bfloat16)
        return inside.at[lower_ids].set(keep)
    owned = jax.vmap(owned_mask)(domain_ids, left_ids)

    def accumulate(total, items):
        block, marks = items
        masked = block * marks[None, :]
        part = lax.dot_general(masked, block, (((1,), (1,)), ((), ())), preferred_element_type=jnp.float32)
        return (total + part, 0)
    gram = lax.scan(accumulate, jnp.zeros((NS, NS), jnp.float32), (current, owned))[0]
    coeffs = inverse_root(gram)

    def rotate(block):
        return lax.dot_general(coeffs, block, (((0,), (0,)), ((), ())), preferred_element_type=jnp.float32).astype(jnp.bfloat16)
    rotated = lax.map(rotate, current)
    return rotated.transpose(1, 0, 2).reshape(NS, DOMS * LNP)
```

```python
import functools
import jax
import jax.numpy as jnp
from jax import lax
from jax.experimental import pallas as pl
from jax.experimental.pallas import tpu as pltpu
from jax.sharding import PartitionSpec as P

DEGREE = 3
NS_ITERS = 3
LN = 3480
LANES = 128
BATCH = 16


def passed_along(x, axis, by):
    devices = lax.axis_size(axis)
    pairs = [(i, i + by) for i in range(devices) if 0 <= i + by < devices]
    return lax.ppermute(x, axis, pairs)


def inverse_root(gram):
    frobenius = jnp.sqrt(jnp.sum(gram * gram) + 1e-06)
    iterate = gram / frobenius
    identity = jnp.eye(gram.shape[0], dtype=jnp.float32)
    inverse = identity
    for sweep in range(NS_ITERS):
        factor = 1.5 * identity - 0.5 * jnp.dot(inverse, iterate, precision=lax.Precision.HIGHEST)
        iterate = jnp.dot(iterate, factor, precision=lax.Precision.HIGHEST)
        inverse = jnp.dot(factor, inverse, precision=lax.Precision.HIGHEST)
    return (inverse / jnp.sqrt(frobenius)).astype(jnp.bfloat16)


def batches(count, body):
    whole, rest = divmod(count, BATCH)

    def step(g, carry):
        body(pl.multiple_of(g * BATCH, BATCH), BATCH)
        return carry

    lax.fori_loop(0, whole, step, 0)
    if rest:
        body(whole * BATCH, rest)


def add_faces(field, faces, wide, ids, scale):
    count = ids.shape[1]
    tiles = field.shape[1] and wide.shape[0] // count
    for side in range(2):
        wide[...] = faces[side].astype(jnp.float32) * scale

        def add(base, size):
            rows = [pl.ds(ids[side, base + i] * tiles, tiles) for i in range(size)]
            old = [field[row, :] for row in rows]
            new = [old[i] + wide[pl.ds((base + i) * tiles, tiles), :] for i in range(size)]
            for i in range(size):
                field[rows[i], :] = new[i]

        batches(count, add)


def apply_kernel(first, *refs):
    if first:
        (conn, ids, scales, coef, pot_rows, pot, stiff, start,
         out, rounded, faces, field, total, gathered, products, wide) = refs
    else:
        (conn, ids, scales, coef, pot_rows, pot, stiff, before, older, came,
         out, rounded, faces, field, total, gathered, products, wide) = refs
    cells, dofs = conn.shape
    count = ids.shape[1]
    tiles = gathered.shape[0] // dofs
    nodes = field.shape[0] // tiles
    if first:
        width = 512
        for k in range(nodes // width):
            piece = start[:, k * width:(k + 1) * width].astype(jnp.float32)
            node = lax.broadcasted_iota(jnp.int32, piece.shape, 1) + k * width
            turned = jnp.where(node < LN, piece, 0.0).T
            for j in range(tiles):
                field[pl.ds(k * width * tiles + j, width, tiles), :] = turned[:, j * LANES:(j + 1) * LANES]
    else:
        field[...] = before[...]
        add_faces(field, came, wide, ids, coef[2])
        field[...] = field[...].astype(jnp.bfloat16).astype(jnp.float32)
    rounded[...] = field[...].astype(jnp.bfloat16)
    total[...] = pot[...] * field[...]

    def gather(cell, base):
        for i in range(BATCH):
            row = conn[cell, base + i] * tiles
            gathered[pl.ds((base + i) * tiles, tiles), :] = field[pl.ds(row, tiles), :]

    def scatter(cell, base):
        rows = [pl.ds(conn[cell, base + i] * tiles, tiles) for i in range(BATCH)]
        old = [total[row, :] for row in rows]
        new = [old[i] + products[pl.ds((base + i) * tiles, tiles), :] for i in range(BATCH)]
        for i in range(BATCH):
            total[rows[i], :] = new[i]

    def one_cell(cell, carry):
        def get(g, c):
            gather(cell, pl.multiple_of(g * BATCH, BATCH))
            return c

        lax.fori_loop(0, dofs // BATCH, get, 0)
        values = jnp.concatenate(
            [gathered[pl.ds(j, dofs, tiles), :].astype(jnp.bfloat16) for j in range(tiles)], axis=1)
        result = jnp.dot(stiff[...], values, preferred_element_type=jnp.float32) * scales[cell]
        for j in range(tiles):
            products[pl.ds(j, dofs, tiles), :] = result[:, j * LANES:(j + 1) * LANES]

        def put(g, c):
            scatter(cell, pl.multiple_of(g * BATCH, BATCH))
            return c

        lax.fori_loop(0, dofs // BATCH, put, 0)
        return carry

    lax.fori_loop(0, cells, one_cell, 0)

    for side in range(2):
        def take(base, size):
            for i in range(size):
                wide[pl.ds((base + i) * tiles, tiles), :] = total[pl.ds(ids[side, base + i] * tiles, tiles), :]

        batches(count, take)
        faces[side] = wide[...].astype(faces.dtype)
    value = coef[1] * (total[...] - coef[0] * field[...])
    if not first:
        value = value - older[...].astype(jnp.float32)
    out[...] = value


def finish_kernel(ids, coef, before, came, out, field, wide):
    count = ids.shape[1]
    tiles = wide.shape[0] // count
    nodes = field.shape[0] // tiles
    field[...] = before[...]
    add_faces(field, came, wide, ids, coef[2])
    width = 512
    for k in range(nodes // width):
        piece = jnp.concatenate(
            [field[pl.ds(k * width * tiles + j, width, tiles), :] for j in range(tiles)], axis=1)
        out[:, k * width:(k + 1) * width] = piece.T.astype(jnp.bfloat16)


SMEM = pl.BlockSpec(memory_space=pltpu.SMEM)
VMEM = pl.BlockSpec(memory_space=pltpu.VMEM)


def apply_call(first, conn, ids, scales, coef, pot, stiff, *fields):
    cells, dofs = conn.shape
    count = ids.shape[1]
    rows = pot.shape[0]
    f32, bf16 = jnp.float32, jnp.bfloat16
    states = fields[0].shape[0] if first else None
    tiles = states // LANES if first else fields[2].shape[1] // count
    out_shape = (
        jax.ShapeDtypeStruct((rows, LANES), f32),
        jax.ShapeDtypeStruct((rows, LANES), bf16),
        jax.ShapeDtypeStruct((2, count * tiles, LANES), bf16),
    )
    return pl.pallas_call(
        functools.partial(apply_kernel, first),
        out_shape=out_shape,
        in_specs=[SMEM] * 4 + [SMEM] + [VMEM] * (2 + len(fields)),
        out_specs=[VMEM] * 3,
        scratch_shapes=[
            pltpu.VMEM((rows, LANES), f32),
            pltpu.VMEM((rows, LANES), f32),
            pltpu.VMEM((dofs * tiles, LANES), f32),
            pltpu.VMEM((dofs * tiles, LANES), f32),
            pltpu.VMEM((count * tiles, LANES), f32),
        ],
        compiler_params=pltpu.CompilerParams(vmem_limit_bytes=40 * 1024 * 1024),
    )(conn, ids, scales, coef, coef, pot, stiff, *fields)


def body(start_states, stiffness, cell_scale, potential, connectivity, shared_nodes, filter_bounds):
    nodes = start_states.shape[1]
    block_states = start_states.shape[0]
    tiles = pl.cdiv(block_states, LANES)
    states = tiles * LANES
    start_states = jnp.pad(start_states, ((0, states - block_states), (0, 0)))
    rows = nodes * tiles
    ids = shared_nodes[0]
    pot = jnp.broadcast_to(potential[:, None, None], (nodes, tiles, LANES)).reshape(rows, LANES)
    stiff = stiffness.T
    center = (filter_bounds[1] + filter_bounds[0]) / 2.0
    inv = 2.0 / (filter_bounds[1] - filter_bounds[0])

    def exchange(faces):
        below = passed_along(faces[1], "dom", 1)
        above = passed_along(faces[0], "dom", -1)
        return jnp.stack([below, above])

    first = jnp.stack([center, inv, inv])
    second = jnp.stack([center, 2 * inv, inv])
    later = jnp.stack([center, 2 * inv, 2 * inv])
    value, older, faces = apply_call(True, connectivity, ids, cell_scale, first, pot, stiff, start_states)
    for degree_step in range(DEGREE - 1):
        coef = second if degree_step == 0 else later
        value, newer, faces = apply_call(
            False, connectivity, ids, cell_scale, coef, pot, stiff, value, older, exchange(faces))
        older = newer
    current = pl.pallas_call(
        finish_kernel,
        out_shape=jax.ShapeDtypeStruct((states, nodes), jnp.bfloat16),
        in_specs=[SMEM, SMEM, VMEM, VMEM],
        out_specs=VMEM,
        scratch_shapes=[pltpu.VMEM((rows, LANES), jnp.float32),
                        pltpu.VMEM((ids.shape[1] * tiles, LANES), jnp.float32)],
        compiler_params=pltpu.CompilerParams(vmem_limit_bytes=40 * 1024 * 1024),
    )(ids, later, value, exchange(faces))[:block_states]
    left_ids = ids[0]
    inside = (jnp.arange(nodes) < LN).astype(jnp.bfloat16)
    keep = jnp.where(lax.axis_index("dom") > 0, 0.0, 1.0).astype(jnp.bfloat16)
    owned = inside.at[left_ids].set(keep)
    masked = current * owned[None, :]
    partial_rows = lax.dot_general(
        masked,
        lax.all_gather(current, "st", axis=0, tiled=True),
        (((1,), (1,)), ((), ())),
        preferred_element_type=jnp.float32,
    )
    summed_rows = lax.psum(partial_rows, "dom")
    gram = lax.all_gather(summed_rows, "st", axis=0, tiled=True)
    coeffs = inverse_root(gram)
    columns = lax.dynamic_slice_in_dim(coeffs, lax.axis_index("st") * block_states, block_states, 1)
    rotated = lax.dot_general(
        columns,
        lax.all_gather(current, "st", axis=0, tiled=True),
        (((0,), (0,)), ((), ())),
        preferred_element_type=jnp.float32,
    )
    return rotated.astype(jnp.bfloat16)


def solution(mesh):
    placed = (P("st", "dom"), P(), P("dom"), P("dom"), P("dom", None), P("dom", None, None), P())
    return jax.shard_map(
        body, mesh=mesh, in_specs=placed, out_specs=P("st", "dom"), check_vma=False
    )
```

```python
import functools
import jax
import jax.numpy as jnp
from jax import lax
from jax.experimental import pallas as pl
from jax.experimental.pallas import tpu as pltpu
from jax.sharding import PartitionSpec as P

DEGREE = 3
NS_ITERS = 3
LN = 3480
LANES = 128
BATCH = 16


def passed_along(x, axis, by):
    devices = lax.axis_size(axis)
    pairs = [(i, i + by) for i in range(devices) if 0 <= i + by < devices]
    return lax.ppermute(x, axis, pairs)


def inverse_root(gram):
    frobenius = jnp.sqrt(jnp.sum(gram * gram) + 1e-06)
    iterate = gram / frobenius
    identity = jnp.eye(gram.shape[0], dtype=jnp.float32)
    inverse = identity
    for sweep in range(NS_ITERS):
        factor = 1.5 * identity - 0.5 * jnp.dot(inverse, iterate, precision=lax.Precision.HIGHEST)
        iterate = jnp.dot(iterate, factor, precision=lax.Precision.HIGHEST)
        inverse = jnp.dot(factor, inverse, precision=lax.Precision.HIGHEST)
    return (inverse / jnp.sqrt(frobenius)).astype(jnp.bfloat16)


def batches(count, body):
    whole, rest = divmod(count, BATCH)

    def step(g, carry):
        body(pl.multiple_of(g * BATCH, BATCH), BATCH)
        return carry

    lax.fori_loop(0, whole, step, 0)
    if rest:
        body(whole * BATCH, rest)


def add_faces(field, faces, wide, ids, scale):
    count = ids.shape[0] // 2
    tiles = wide.shape[0] // count
    for side in range(2):
        wide[...] = faces[side].astype(jnp.float32) * scale

        def add(base, size):
            rows = [pl.ds(ids[side * count + base + i], tiles) for i in range(size)]
            old = [field[row, :] for row in rows]
            new = [old[i] + wide[pl.ds((base + i) * tiles, tiles), :] for i in range(size)]
            for i in range(size):
                field[rows[i], :] = new[i]

        batches(count, add)


def apply_kernel(first, *refs):
    if first:
        (conn, ids, scales, coef, pot, stiff, start,
         out, rounded, faces, field, total, gathered, products, wide) = refs
    else:
        (conn, ids, scales, coef, pot, stiff, before, older, came,
         out, rounded, faces, field, total, gathered, products, wide) = refs
    dofs = stiff.shape[0]
    cells = conn.shape[0] // dofs
    count = ids.shape[0] // 2
    tiles = gathered.shape[0] // dofs
    nodes = field.shape[0] // tiles
    if first:
        width = 512
        for k in range(nodes // width):
            piece = start[:, k * width:(k + 1) * width].astype(jnp.float32)
            node = lax.broadcasted_iota(jnp.int32, piece.shape, 1) + k * width
            turned = jnp.where(node < LN, piece, 0.0).T
            for j in range(tiles):
                field[pl.ds(k * width * tiles + j, width, tiles), :] = turned[:, j * LANES:(j + 1) * LANES]
    else:
        field[...] = before[...]
        add_faces(field, came, wide, ids, coef[2])
        field[...] = field[...].astype(jnp.bfloat16).astype(jnp.float32)
    rounded[...] = field[...].astype(jnp.bfloat16)
    total[...] = pot[...] * field[...]

    def gather(cell, base):
        for i in range(BATCH):
            row = conn[cell * dofs + base + i]
            gathered[pl.ds((base + i) * tiles, tiles), :] = field[pl.ds(row, tiles), :]

    def scatter(cell, base):
        rows = [pl.ds(conn[cell * dofs + base + i], tiles) for i in range(BATCH)]
        old = [total[row, :] for row in rows]
        new = [old[i] + products[pl.ds((base + i) * tiles, tiles), :] for i in range(BATCH)]
        for i in range(BATCH):
            total[rows[i], :] = new[i]

    def one_cell(cell, carry):
        def get(g, c):
            gather(cell, pl.multiple_of(g * BATCH, BATCH))
            return c

        lax.fori_loop(0, dofs // BATCH, get, 0)
        values = jnp.concatenate(
            [gathered[pl.ds(j, dofs, tiles), :].astype(jnp.bfloat16) for j in range(tiles)], axis=1)
        result = jnp.dot(stiff[...], values, preferred_element_type=jnp.float32) * scales[cell]
        for j in range(tiles):
            products[pl.ds(j, dofs, tiles), :] = result[:, j * LANES:(j + 1) * LANES]

        def put(g, c):
            scatter(cell, pl.multiple_of(g * BATCH, BATCH))
            return c

        lax.fori_loop(0, dofs // BATCH, put, 0)
        return carry

    lax.fori_loop(0, cells, one_cell, 0)

    for side in range(2):
        def take(base, size):
            for i in range(size):
                wide[pl.ds((base + i) * tiles, tiles), :] = total[pl.ds(ids[side * count + base + i], tiles), :]

        batches(count, take)
        faces[side] = wide[...].astype(faces.dtype)
    value = coef[1] * (total[...] - coef[0] * field[...])
    if not first:
        value = value - older[...].astype(jnp.float32)
    out[...] = value


def finish_kernel(ids, coef, part, before, came, owned, out, own_half, other_half, gram, field, wide):
    count = ids.shape[0] // 2
    tiles = wide.shape[0] // count
    states, nodes = out.shape
    half = nodes // 2
    field[...] = before[...]
    add_faces(field, came, wide, ids, coef[2])
    width = 512
    for k in range(nodes // width):
        piece = jnp.concatenate(
            [field[pl.ds(k * width * tiles + j, width, tiles), :] for j in range(tiles)], axis=1)
        out[:, k * width:(k + 1) * width] = piece.T.astype(jnp.bfloat16)
    start = pl.multiple_of(part[0] * half, LANES)
    away = pl.multiple_of((1 - part[0]) * half, LANES)
    own_half[...] = out[:, pl.ds(start, half)]
    other_half[...] = out[:, pl.ds(away, half)]
    gram[...] = lax.dot_general(
        out[...] * owned[...], out[...], (((1,), (1,)), ((), ())), preferred_element_type=jnp.float32)


def cross_kernel(part, mine, came, owned, out):
    half = mine.shape[1]
    start = pl.multiple_of(part[0] * half, LANES)
    masked = mine[...] * owned[:, pl.ds(start, half)]
    dims = (((1,), (1,)), ((), ()))

    @pl.when(part[0] == 0)
    def _():
        out[...] = lax.dot_general(masked, came[...], dims, preferred_element_type=jnp.float32)

    @pl.when(part[0] != 0)
    def _():
        out[...] = lax.dot_general(came[...], masked, dims, preferred_element_type=jnp.float32)


def split(x):
    high = x.astype(jnp.bfloat16)
    return high, (x - high.astype(jnp.float32)).astype(jnp.bfloat16)


def product(a, b):
    def dot(x, y):
        return jnp.dot(x, y, preferred_element_type=jnp.float32)

    return dot(a[0], b[0]) + (dot(a[0], b[1]) + dot(a[1], b[0]))


def root_kernel(part, blocks, out, gram, held):
    size = blocks.shape[1]
    cross = blocks[2]
    gram[:size, :size] = blocks[0]
    gram[size:, size:] = blocks[1]
    gram[:size, size:] = cross
    gram[size:, :size] = cross.T
    whole = gram[...]
    scale = jnp.sqrt(jnp.sum(whole * whole, keepdims=True) + 1e-06)
    start = pl.multiple_of(part[0] * size, LANES)
    row = lax.broadcasted_iota(jnp.int32, whole.shape, 0)
    column = lax.broadcasted_iota(jnp.int32, whole.shape, 1)
    diagonal = jnp.where(row == column, 1.5, 0.0)
    iterate = split(whole / scale)
    factor = diagonal - 0.5 * (whole / scale)
    inverse = split(factor)
    for sweep in range(1, NS_ITERS):
        iterate = split(product(iterate, split(factor)))
        factor = diagonal - 0.5 * product(inverse, iterate)
        if sweep == NS_ITERS - 1:
            held[0] = inverse[0]
            held[1] = inverse[1]
            columns = held[0, :, pl.ds(start, size)], held[1, :, pl.ds(start, size)]
            result = product(split(factor), columns)
        else:
            inverse = split(product(split(factor), inverse))
    out[...] = (result / jnp.sqrt(scale)).astype(jnp.bfloat16)


def rotate_kernel(part, columns, mine, first, rest_a, rest_b, out):
    states, nodes = out.shape
    half = nodes // 2
    dims = (((0,), (0,)), ((), ()))
    own = columns[pl.ds(pl.multiple_of(part[0] * states, states), states), :]
    other = columns[pl.ds(pl.multiple_of((1 - part[0]) * states, states), states), :]

    def part_of(base, came):
        width = came.shape[1]
        value = lax.dot_general(own, mine[:, pl.ds(base, width)], dims, preferred_element_type=jnp.float32)
        value += lax.dot_general(other, came[...], dims, preferred_element_type=jnp.float32)
        out[:, pl.ds(base, width)] = value.astype(out.dtype)

    part_of(pl.multiple_of(part[0] * half, LANES), first)
    away = (1 - part[0]) * half
    part_of(pl.multiple_of(away, LANES), rest_a)
    part_of(pl.multiple_of(away + rest_a.shape[1], LANES), rest_b)


SMEM = pl.BlockSpec(memory_space=pltpu.SMEM)
VMEM = pl.BlockSpec(memory_space=pltpu.VMEM)
LIMIT = pltpu.CompilerParams(vmem_limit_bytes=40 * 1024 * 1024)


def apply_call(first, conn, ids, scales, coef, pot, stiff, *fields):
    dofs = stiff.shape[0]
    count = ids.shape[0] // 2
    rows = pot.shape[0]
    f32, bf16 = jnp.float32, jnp.bfloat16
    tiles = fields[0].shape[0] // LANES if first else fields[2].shape[1] // count
    out_shape = (
        jax.ShapeDtypeStruct((rows, LANES), f32),
        jax.ShapeDtypeStruct((rows, LANES), bf16),
        jax.ShapeDtypeStruct((2, count * tiles, LANES), bf16),
    )
    return pl.pallas_call(
        functools.partial(apply_kernel, first),
        out_shape=out_shape,
        in_specs=[SMEM] * 4 + [VMEM] * (2 + len(fields)),
        out_specs=[VMEM] * 3,
        scratch_shapes=[
            pltpu.VMEM((rows, LANES), f32),
            pltpu.VMEM((rows, LANES), f32),
            pltpu.VMEM((dofs * tiles, LANES), f32),
            pltpu.VMEM((dofs * tiles, LANES), f32),
            pltpu.VMEM((count * tiles, LANES), f32),
        ],
        compiler_params=LIMIT,
        name="apply",
    )(conn, ids, scales, coef, pot, stiff, *fields)


def groups_of(devices):
    bits = devices.bit_length() - 1
    return [list(range(b, min(b + 2, bits))) if b else [0] for b in [0] + list(range(1, bits, 2))][:bits]


def plan(group):
    for m in range(1, 1 << len(group)):
        yield m, sum(((m >> i) & 1) << bit for i, bit in enumerate(group))


def code_of(group):
    at = lax.axis_index("dom")
    return sum(((at >> bit) & 1) << i for i, bit in enumerate(group))


def sum_scatter(x):
    devices = lax.axis_size("dom")
    for group in groups_of(devices):
        size = x.shape[-2] >> len(group)
        code = code_of(group)
        came = [
            lax.ppermute(
                lax.dynamic_slice_in_dim(x, (code ^ m) * size, size, x.ndim - 2),
                "dom", [(i, i ^ mask) for i in range(devices)])
            for m, mask in plan(group)
        ]
        x = lax.dynamic_slice_in_dim(x, code * size, size, x.ndim - 2)
        for y in came:
            x = x + y
    return x


def gather_all(x):
    devices = lax.axis_size("dom")
    for group in reversed(groups_of(devices)):
        size = x.shape[-2]
        code = code_of(group)
        pieces = [(0, x)] + [
            (m, lax.ppermute(x, "dom", [(i, i ^ mask) for i in range(devices)])) for m, mask in plan(group)
        ]
        x = jnp.zeros(x.shape[:-2] + (size << len(group), x.shape[-1]), x.dtype)
        for m, piece in pieces:
            x = lax.dynamic_update_slice_in_dim(x, piece, (code ^ m) * size, x.ndim - 2)
    return x


def rotate_pair(current, own_half, other_half, gram, owned, part):
    states, nodes = current.shape
    f32, bf16 = jnp.float32, jnp.bfloat16
    swap = [(0, 1), (1, 0)]
    came = lax.ppermute(other_half, "st", swap)
    own_sum = sum_scatter(gram)
    cross = pl.pallas_call(
        cross_kernel,
        out_shape=jax.ShapeDtypeStruct((states, states), f32),
        in_specs=[SMEM, VMEM, VMEM, VMEM], out_specs=VMEM, compiler_params=LIMIT, name="cross",
    )(part, own_half, came, owned)
    quarter = nodes // 4 // LANES * LANES
    rest, cross = lax.optimization_barrier((own_half, cross))
    rest_a = lax.ppermute(rest[:, :quarter], "st", swap)
    cross_sum = sum_scatter(cross)
    rest_a, cross_sum = lax.optimization_barrier((rest_a, cross_sum))
    pair = jnp.stack([own_sum, cross_sum])
    theirs = lax.ppermute(pair, "st", swap)
    later, theirs = lax.optimization_barrier((rest[:, quarter:], theirs))
    rest_b = lax.ppermute(later, "st", swap)
    lower = part[0] == 0
    blocks = gather_all(jnp.stack([
        jnp.where(lower, pair[0], theirs[0]), jnp.where(lower, theirs[0], pair[0]), pair[1] + theirs[1]]))
    columns = pl.pallas_call(
        root_kernel,
        out_shape=jax.ShapeDtypeStruct((2 * states, states), bf16),
        in_specs=[SMEM, VMEM], out_specs=VMEM,
        scratch_shapes=[pltpu.VMEM((2 * states, 2 * states), f32), pltpu.VMEM((2, 2 * states, 2 * states), bf16)],
        compiler_params=LIMIT, name="root",
    )(part, blocks)
    return pl.pallas_call(
        rotate_kernel,
        out_shape=jax.ShapeDtypeStruct((states, nodes), bf16),
        in_specs=[SMEM] + [VMEM] * 5, out_specs=VMEM, compiler_params=LIMIT, name="rotate",
    )(part, columns, current, came, rest_a, rest_b)


def rotate_any(current, owned):
    states = current.shape[0]
    whole = lax.all_gather(current, "st", axis=0, tiled=True)
    rows = lax.dot_general(
        current * owned, whole, (((1,), (1,)), ((), ())), preferred_element_type=jnp.float32)
    gram = lax.all_gather(lax.psum(rows, "dom"), "st", axis=0, tiled=True)
    columns = lax.dynamic_slice_in_dim(inverse_root(gram), lax.axis_index("st") * states, states, 1)
    rotated = lax.dot_general(
        columns, whole, (((0,), (0,)), ((), ())), preferred_element_type=jnp.float32)
    return rotated.astype(jnp.bfloat16)


def body(start_states, stiffness, cell_scale, potential, connectivity, shared_nodes, filter_bounds):
    block_states, nodes = start_states.shape
    tiles = pl.cdiv(block_states, LANES)
    states = tiles * LANES
    start_states = jnp.pad(start_states, ((0, states - block_states), (0, 0)))
    rows = nodes * tiles
    conn = connectivity.reshape(-1) * tiles
    ids = shared_nodes.reshape(-1) * tiles
    pot = jnp.broadcast_to(potential[:, None, None], (nodes, tiles, LANES)).reshape(rows, LANES)
    stiff = stiffness.T
    center = (filter_bounds[1] + filter_bounds[0]) / 2.0
    inv = 2.0 / (filter_bounds[1] - filter_bounds[0])
    part = lax.axis_index("st").reshape(1)
    inside = (jnp.arange(nodes) < LN).astype(jnp.bfloat16)
    keep = jnp.where(lax.axis_index("dom") > 0, 0.0, 1.0).astype(jnp.bfloat16)
    owned = inside.at[shared_nodes[0, 0]].set(keep)[None, :]

    def exchange(faces):
        below = passed_along(faces[1], "dom", 1)
        above = passed_along(faces[0], "dom", -1)
        return jnp.stack([below, above])

    first = jnp.stack([center, inv, inv])
    second = jnp.stack([center, 2 * inv, inv])
    later = jnp.stack([center, 2 * inv, 2 * inv])
    value, older, faces = apply_call(True, conn, ids, cell_scale, first, pot, stiff, start_states)
    for degree_step in range(DEGREE - 1):
        coef = second if degree_step == 0 else later
        value, newer, faces = apply_call(
            False, conn, ids, cell_scale, coef, pot, stiff, value, older, exchange(faces))
        older = newer
    half = jax.ShapeDtypeStruct((states, nodes // 2), jnp.bfloat16)
    current, own_half, other_half, gram = pl.pallas_call(
        finish_kernel,
        out_shape=(jax.ShapeDtypeStruct((states, nodes), jnp.bfloat16), half, half,
                   jax.ShapeDtypeStruct((states, states), jnp.float32)),
        in_specs=[SMEM] * 3 + [VMEM] * 3,
        out_specs=[VMEM] * 4,
        scratch_shapes=[pltpu.VMEM((rows, LANES), jnp.float32),
                        pltpu.VMEM((ids.shape[0] // 2 * tiles, LANES), jnp.float32)],
        compiler_params=LIMIT,
        name="finish",
    )(ids, later, part, value, exchange(faces), owned)
    devices = lax.axis_size("dom")
    if lax.axis_size("st") == 2 and states == block_states and devices & (devices - 1) == 0:
        return rotate_pair(current, own_half, other_half, gram, owned, part)
    return rotate_any(current[:block_states], owned)


def solution(mesh):
    placed = (P("st", "dom"), P(), P("dom"), P("dom"), P("dom", None), P("dom", None, None), P())
    return jax.shard_map(
        body, mesh=mesh, in_specs=placed, out_specs=P("st", "dom"), check_vma=False
    )
```

```python
import functools
import jax
import jax.numpy as jnp
from jax import lax
from jax.experimental import pallas as pl
from jax.experimental.pallas import tpu as pltpu
from jax.sharding import PartitionSpec as P

DEGREE = 3
NS_ITERS = 3
LN = 3480
LANES = 128
BATCH = 32
SPAN = 256
WIDTH = 256


def passed_along(x, axis, by):
    devices = lax.axis_size(axis)
    pairs = [(i, i + by) for i in range(devices) if 0 <= i + by < devices]
    return lax.ppermute(x, axis, pairs)


def inverse_root(gram):
    frobenius = jnp.sqrt(jnp.sum(gram * gram) + 1e-06)
    iterate = gram / frobenius
    identity = jnp.eye(gram.shape[0], dtype=jnp.float32)
    inverse = identity
    for sweep in range(NS_ITERS):
        factor = 1.5 * identity - 0.5 * jnp.dot(inverse, iterate, precision=lax.Precision.HIGHEST)
        iterate = jnp.dot(iterate, factor, precision=lax.Precision.HIGHEST)
        inverse = jnp.dot(factor, inverse, precision=lax.Precision.HIGHEST)
    return (inverse / jnp.sqrt(frobenius)).astype(jnp.bfloat16)


def batches(count, size, body):
    whole, rest = divmod(count, size)

    def step(g, carry):
        body(pl.multiple_of(g * size, size), size)
        return carry

    lax.fori_loop(0, whole, step, 0)
    if rest:
        body(whole * size, rest)


def add_faces(field, came, wide, ids, scale):
    count = ids.shape[0] // 2
    tiles = wide.shape[0] // count
    for side in range(2):
        wide[...] = came[side][...].astype(jnp.float32) * scale

        def add(base, size):
            rows = [pl.ds(ids[side * count + base + i], tiles) for i in range(size)]
            old = [field[row, :] for row in rows]
            new = [old[i] + wide[pl.ds((base + i) * tiles, tiles), :] for i in range(size)]
            for i in range(size):
                field[rows[i], :] = new[i]

        batches(count, BATCH, add)


def slope(bounds, times):
    return (2.0 * times) / jnp.full((1, LANES), bounds[1] - bounds[0], jnp.float32)


def apply_kernel(step, *refs):
    if step == 0:
        (conn, ids, scales, bounds, pot_row, stiff, start,
         field, rounded, below, above, pot, total, gathered, products, wide) = refs
    else:
        (conn, ids, scales, bounds, pot, stiff, before, older, came_low, came_high,
         field, rounded, below, above, total, gathered, products, wide) = refs
    dofs = stiff.shape[0]
    cells = conn.shape[0] // dofs
    count = ids.shape[0] // 2
    tiles = gathered.shape[0] // dofs
    nodes = field.shape[0] // tiles
    if step == 0:
        width = 512
        for k in range(nodes // width):
            piece = start[:, k * width:(k + 1) * width].astype(jnp.float32)
            node = lax.broadcasted_iota(jnp.int32, piece.shape, 1) + k * width
            turned = jnp.where(node < LN, piece, 0.0).T
            spread = jnp.broadcast_to(pot_row[:, k * width:(k + 1) * width], (LANES, width)).T
            for j in range(tiles):
                field[pl.ds(k * width * tiles + j, width, tiles), :] = turned[:, j * LANES:(j + 1) * LANES]
                pot[pl.ds(k * width * tiles + j, width, tiles), :] = spread
    else:
        add_faces(field, (came_low, came_high), wide, ids, slope(bounds, min(step, 2)))

    def begin(g, carry):
        rows = pl.ds(pl.multiple_of(g * SPAN, SPAN), SPAN)
        low = field[rows, :].astype(jnp.bfloat16)
        rounded[rows, :] = low
        total[rows, :] = pot[rows, :] * low.astype(jnp.float32)
        return carry

    lax.fori_loop(0, field.shape[0] // SPAN, begin, 0)

    def gather(cell, base, size):
        for i in range(size):
            row = conn[cell * dofs + base + i]
            gathered[pl.ds((base + i) * tiles, tiles), :] = field[pl.ds(row, tiles), :]

    def scatter_and_gather(cell, following, base, size):
        rows = [pl.ds(conn[cell * dofs + base + i], tiles) for i in range(size)]
        old = [total[row, :] for row in rows]
        new = [old[i] + products[pl.ds((base + i) * tiles, tiles), :] for i in range(size)]
        for i in range(size):
            total[rows[i], :] = new[i]
        gather(following, base, size)

    batches(dofs, BATCH, functools.partial(gather, 0))

    def one_cell(cell, carry):
        values = jnp.concatenate(
            [gathered[pl.ds(j, dofs, tiles), :].astype(jnp.bfloat16) for j in range(tiles)], axis=1)
        result = jnp.dot(stiff[...], values, preferred_element_type=jnp.float32) * scales[cell]
        for j in range(tiles):
            products[pl.ds(j, dofs, tiles), :] = result[:, j * LANES:(j + 1) * LANES]
        following = jnp.minimum(cell + 1, cells - 1)
        batches(dofs, BATCH, functools.partial(scatter_and_gather, cell, following))
        return carry

    lax.fori_loop(0, cells, one_cell, 0)

    for side, faces in enumerate((below, above)):
        def take(base, size):
            for i in range(size):
                wide[pl.ds((base + i) * tiles, tiles), :] = total[pl.ds(ids[side * count + base + i], tiles), :]

        batches(count, BATCH, take)
        faces[...] = wide[...].astype(faces.dtype)
    center = (bounds[1] + bounds[0]) * 0.5
    rate = slope(bounds, min(step + 1, 2))

    def end(g, carry):
        rows = pl.ds(pl.multiple_of(g * SPAN, SPAN), SPAN)
        value = rate * (total[rows, :] - center * rounded[rows, :].astype(jnp.float32))
        if step:
            value = value - older[rows, :].astype(jnp.float32)
        field[rows, :] = value
        return carry

    lax.fori_loop(0, field.shape[0] // SPAN, end, 0)


def node_rows(field, start, width, tiles):
    return jnp.concatenate(
        [field[pl.ds(start * tiles + j, width, tiles), :] for j in range(tiles)], axis=1)


def send_kernel(ids, bounds, at, before, came_low, came_high, field, away, wide):
    count = ids.shape[0] // 2
    tiles = wide.shape[0] // count
    half = away.shape[0]
    add_faces(field, (came_low, came_high), wide, ids, slope(bounds, 2))
    start = (1 - at[0]) * half
    width = WIDTH
    for k in range(half // width):
        away[k * width:(k + 1) * width, :] = node_rows(
            field, start + k * width, width, tiles).astype(away.dtype)


def turn_kernel(ids, at, before, field, turned, own, own_masked, gram):
    count = ids.shape[0] // 2
    states, nodes = turned.shape
    tiles = states // LANES
    half = own.shape[0]
    start = pl.multiple_of(at[0] * half, LANES)
    width = WIDTH
    for k in range(half // width):
        own[k * width:(k + 1) * width, :] = node_rows(
            field, start + k * width, width, tiles).astype(own.dtype)
    for k in range(nodes // width):
        turned[:, k * width:(k + 1) * width] = node_rows(field, k * width, width, tiles).T.astype(turned.dtype)

    @pl.when(at[1] > 0)
    def _():
        def drop(base, size):
            for i in range(size):
                field[pl.ds(ids[base + i], tiles), :] = jnp.zeros((tiles, LANES), jnp.float32)

        batches(count, BATCH, drop)

    for k in range(half // width):
        own_masked[:, k * width:(k + 1) * width] = node_rows(
            field, start + k * width, width, tiles).T.astype(own_masked.dtype)
    total = jnp.zeros(gram.shape, jnp.float32)
    for k in range(nodes // width):
        total += jnp.dot(turned[:, k * width:(k + 1) * width],
                         node_rows(field, k * width, width, tiles).astype(turned.dtype),
                         preferred_element_type=jnp.float32)
    gram[...] = total


def cross_kernel(at, mine, came, out):
    value = jnp.dot(mine[...], came[...], preferred_element_type=jnp.float32)

    @pl.when(at[0] == 0)
    def _():
        out[...] = value

    @pl.when(at[0] != 0)
    def _():
        out[...] = value.T


def split(x):
    high = x.astype(jnp.bfloat16)
    return high, (x - high.astype(jnp.float32)).astype(jnp.bfloat16)


def product(a, b):
    def dot(x, y):
        return jnp.dot(x, y, preferred_element_type=jnp.float32)

    return dot(a[0], b[0]) + (dot(a[0], b[1]) + dot(a[1], b[0]))


def root_kernel(at, blocks, out, gram, held):
    size = blocks.shape[1]
    cross = blocks[2]
    gram[:size, :size] = blocks[0]
    gram[size:, size:] = blocks[1]
    gram[:size, size:] = cross
    gram[size:, :size] = cross.T
    whole = gram[...]
    scale = jnp.sqrt(jnp.sum(whole * whole, keepdims=True) + 1e-06)
    start = pl.multiple_of(at[0] * size, LANES)
    row = lax.broadcasted_iota(jnp.int32, whole.shape, 0)
    column = lax.broadcasted_iota(jnp.int32, whole.shape, 1)
    diagonal = jnp.where(row == column, 1.5, 0.0)
    iterate = split(whole / scale)
    factor = diagonal - 0.5 * (whole / scale)
    inverse = split(factor)
    for sweep in range(1, NS_ITERS):
        iterate = split(product(iterate, split(factor)))
        factor = diagonal - 0.5 * product(inverse, iterate)
        if sweep == NS_ITERS - 1:
            held[0] = inverse[0]
            held[1] = inverse[1]
            columns = held[0, :, pl.ds(start, size)], held[1, :, pl.ds(start, size)]
            result = product(split(factor), columns)
        else:
            inverse = split(product(split(factor), inverse))
    out[...] = (result / jnp.sqrt(scale)).astype(jnp.bfloat16)


def rotate_kernel(at, columns, turned, first, rest_a, rest_b, out):
    states, nodes = out.shape
    half = nodes // 2
    own = columns[pl.ds(pl.multiple_of(at[0] * states, states), states), :]
    other = columns[pl.ds(pl.multiple_of((1 - at[0]) * states, states), states), :]

    def part_of(base, came):
        width = came.shape[0]
        base = pl.multiple_of(base, LANES)
        value = lax.dot_general(
            own, turned[:, pl.ds(base, width)], (((0,), (0,)), ((), ())), preferred_element_type=jnp.float32)
        value += lax.dot_general(
            other, came[...], (((0,), (1,)), ((), ())), preferred_element_type=jnp.float32)
        out[:, pl.ds(base, width)] = value.astype(out.dtype)

    part_of(at[0] * half, first)
    away = (1 - at[0]) * half
    part_of(away, rest_a)
    part_of(away + rest_a.shape[0], rest_b)


SMEM = pl.BlockSpec(memory_space=pltpu.SMEM)
VMEM = pl.BlockSpec(memory_space=pltpu.VMEM)
def limit(mib):
    return pltpu.CompilerParams(vmem_limit_bytes=mib * 1024 * 1024)


def struct(shape, dtype=jnp.float32):
    return jax.ShapeDtypeStruct(shape, dtype)


def apply_call(step, tables, pot, stiff, *fields):
    conn, ids = tables[:2]
    dofs = stiff.shape[0]
    count = ids.shape[0] // 2
    f32, bf16 = jnp.float32, jnp.bfloat16
    if step == 0:
        tiles = fields[0].shape[0] // LANES
        rows = fields[0].shape[1] * tiles
    else:
        rows = pot.shape[0]
        tiles = fields[2].shape[0] // count
    face = struct((count * tiles, LANES), bf16)
    out_shape = [struct((rows, LANES)), struct((rows, LANES), bf16), face, face]
    if step == 0:
        out_shape.append(struct((rows, LANES)))
    return pl.pallas_call(
        functools.partial(apply_kernel, step),
        out_shape=out_shape,
        in_specs=[SMEM] * 4 + [VMEM] * (2 + len(fields)),
        out_specs=[VMEM] * len(out_shape),
        scratch_shapes=[
            pltpu.VMEM((rows, LANES), f32),
            pltpu.VMEM((dofs * tiles, LANES), f32),
            pltpu.VMEM((dofs * tiles, LANES), f32),
            pltpu.VMEM((count * tiles, LANES), f32),
        ],
        input_output_aliases={6: 0} if step else {},
        compiler_params=limit(26),
        name="apply",
    )(*tables, pot, stiff, *fields)


def groups_of(devices):
    bits = devices.bit_length() - 1
    return [list(range(b, min(b + 2, bits))) if b else [0] for b in [0] + list(range(1, bits, 2))][:bits]


def plan(group):
    for m in range(1, 1 << len(group)):
        yield m, sum(((m >> i) & 1) << bit for i, bit in enumerate(group))


def code_of(group):
    at = lax.axis_index("dom")
    return sum(((at >> bit) & 1) << i for i, bit in enumerate(group))


def sum_scatter(x):
    devices = lax.axis_size("dom")
    for group in groups_of(devices):
        size = x.shape[-2] >> len(group)
        code = code_of(group)
        came = [
            lax.ppermute(
                lax.dynamic_slice_in_dim(x, (code ^ m) * size, size, x.ndim - 2),
                "dom", [(i, i ^ mask) for i in range(devices)])
            for m, mask in plan(group)
        ]
        x = lax.dynamic_slice_in_dim(x, code * size, size, x.ndim - 2)
        for y in came:
            x = x + y
    return x


def gather_all(x):
    devices = lax.axis_size("dom")
    for group in reversed(groups_of(devices)):
        size = x.shape[-2]
        code = code_of(group)
        pieces = [(0, x)] + [
            (m, lax.ppermute(x, "dom", [(i, i ^ mask) for i in range(devices)])) for m, mask in plan(group)
        ]
        x = jnp.zeros(x.shape[:-2] + (size << len(group), x.shape[-1]), x.dtype)
        for m, piece in pieces:
            x = lax.dynamic_update_slice_in_dim(x, piece, (code ^ m) * size, x.ndim - 2)
    return x


def rotate_pair(field, away, ids, at, states, nodes):
    f32, bf16 = jnp.float32, jnp.bfloat16
    swap = [(0, 1), (1, 0)]
    half = nodes // 2
    came = lax.ppermute(away, "st", swap)
    _, turned, own, own_masked, gram = pl.pallas_call(
        turn_kernel,
        out_shape=[struct(field.shape), struct((states, nodes), bf16), struct((half, states), bf16),
                   struct((states, half), bf16), struct((states, states))],
        in_specs=[SMEM, SMEM, VMEM], out_specs=[VMEM] * 5,
        input_output_aliases={2: 0},
        compiler_params=limit(26), name="turn",
        cost_estimate=pl.CostEstimate(flops=4 * 10**9, bytes_accessed=10**7, transcendentals=0),
    )(ids, at, field)
    own_sum = sum_scatter(gram)
    cross = pl.pallas_call(
        cross_kernel,
        out_shape=struct((states, states)),
        in_specs=[SMEM, VMEM, VMEM], out_specs=VMEM, compiler_params=limit(16), name="cross",
    )(at, own_masked, came)
    first_rows = half // 4 // LANES * LANES
    rest, cross = lax.optimization_barrier((own, cross))
    rest_a = lax.ppermute(rest[:first_rows], "st", swap)
    cross_sum = sum_scatter(cross)
    pair = jnp.stack([own_sum, cross_sum])
    theirs = lax.ppermute(pair, "st", swap)
    later, theirs = lax.optimization_barrier((rest[first_rows:], theirs))
    rest_b = lax.ppermute(later, "st", swap)
    lower = at[0] == 0
    blocks = gather_all(jnp.stack([
        jnp.where(lower, pair[0], theirs[0]), jnp.where(lower, theirs[0], pair[0]), pair[1] + theirs[1]]))
    columns = pl.pallas_call(
        root_kernel,
        out_shape=struct((2 * states, states), bf16),
        in_specs=[SMEM, VMEM], out_specs=VMEM,
        scratch_shapes=[pltpu.VMEM((2 * states, 2 * states), f32), pltpu.VMEM((2, 2 * states, 2 * states), bf16)],
        compiler_params=limit(26), name="root",
    )(at, blocks)
    return pl.pallas_call(
        rotate_kernel,
        out_shape=struct((states, nodes), bf16),
        in_specs=[SMEM] + [VMEM] * 5, out_specs=VMEM, compiler_params=limit(26), name="rotate",
    )(at, columns, turned, came, rest_a, rest_b)


def rotate_any(current, owned):
    states = current.shape[0]
    whole = lax.all_gather(current, "st", axis=0, tiled=True)
    rows = lax.dot_general(
        current * owned, whole, (((1,), (1,)), ((), ())), preferred_element_type=jnp.float32)
    gram = lax.all_gather(lax.psum(rows, "dom"), "st", axis=0, tiled=True)
    columns = lax.dynamic_slice_in_dim(inverse_root(gram), lax.axis_index("st") * states, states, 1)
    rotated = lax.dot_general(
        columns, whole, (((0,), (0,)), ((), ())), preferred_element_type=jnp.float32)
    return rotated.astype(jnp.bfloat16)


def body(start_states, stiffness, cell_scale, potential, connectivity, shared_nodes, filter_bounds):
    block_states, nodes = start_states.shape
    tiles = pl.cdiv(block_states, LANES)
    states = tiles * LANES
    if states != block_states:
        start_states = jnp.pad(start_states, ((0, states - block_states), (0, 0)))
    conn = connectivity.reshape(-1) * tiles
    ids = shared_nodes.reshape(-1) * tiles
    tables = conn, ids, cell_scale, filter_bounds
    stiff = stiffness.T
    at = jnp.stack([lax.axis_index("st"), lax.axis_index("dom")])

    def exchange(low, high):
        return passed_along(high, "dom", 1), passed_along(low, "dom", -1)

    field, older, low, high, pot = apply_call(0, tables, potential[None, :], stiff, start_states)
    for step in range(1, DEGREE):
        field, newer, low, high = apply_call(
            step, tables, pot, stiff, field, older, *exchange(low, high))
        older = newer
    field, away = pl.pallas_call(
        send_kernel,
        out_shape=[struct(field.shape), struct((nodes // 2, states), jnp.bfloat16)],
        in_specs=[SMEM] * 3 + [VMEM] * 3,
        out_specs=[VMEM] * 2,
        scratch_shapes=[pltpu.VMEM((ids.shape[0] // 2 * tiles, LANES), jnp.float32)],
        input_output_aliases={3: 0},
        compiler_params=limit(16),
        name="send",
    )(ids, filter_bounds, at, field, *exchange(low, high))
    devices = lax.axis_size("dom")
    if lax.axis_size("st") == 2 and states == block_states and devices & (devices - 1) == 0:
        return rotate_pair(field, away, ids, at, states, nodes)
    current = field.reshape(nodes, states).T.astype(jnp.bfloat16)[:block_states]
    inside = (jnp.arange(nodes) < LN).astype(jnp.bfloat16)
    keep = jnp.where(lax.axis_index("dom") > 0, 0.0, 1.0).astype(jnp.bfloat16)
    owned = inside.at[shared_nodes[0, 0]].set(keep)[None, :]
    return rotate_any(current, owned)


def solution(mesh):
    placed = (P("st", "dom"), P(), P("dom"), P("dom"), P("dom", None), P("dom", None, None), P())
    return jax.shard_map(
        body, mesh=mesh, in_specs=placed, out_specs=P("st", "dom"), check_vma=False
    )
```

```python
import functools
import jax
import jax.numpy as jnp
from jax import lax
from jax.experimental import pallas as pl
from jax.experimental.pallas import tpu as pltpu
from jax.sharding import PartitionSpec as P

DEGREE = 3
NS_ITERS = 3
LN = 3480
LANES = 128
BATCH = 16
SPAN = 128
WIDTH = 256


def passed_along(x, axis, by):
    devices = lax.axis_size(axis)
    pairs = [(i, i + by) for i in range(devices) if 0 <= i + by < devices]
    return lax.ppermute(x, axis, pairs)


def inverse_root(gram):
    frobenius = jnp.sqrt(jnp.sum(gram * gram) + 1e-06)
    iterate = gram / frobenius
    identity = jnp.eye(gram.shape[0], dtype=jnp.float32)
    inverse = identity
    for sweep in range(NS_ITERS):
        factor = 1.5 * identity - 0.5 * jnp.dot(inverse, iterate, precision=lax.Precision.HIGHEST)
        iterate = jnp.dot(iterate, factor, precision=lax.Precision.HIGHEST)
        inverse = jnp.dot(factor, inverse, precision=lax.Precision.HIGHEST)
    return (inverse / jnp.sqrt(frobenius)).astype(jnp.bfloat16)


def batches(count, size, body):
    whole, rest = divmod(count, size)

    def step(g, carry):
        body(pl.multiple_of(g * size, size), size)
        return carry

    lax.fori_loop(0, whole, step, 0)
    if rest:
        body(whole * size, rest)


def add_faces(field, came, wide, ids, scale, pot=None, total=None):
    count = ids.shape[0] // 2
    tiles = wide.shape[0] // count
    for side in range(2):
        wide[...] = came[side][...].astype(jnp.float32) * scale

        def add(base, size):
            rows = [pl.ds(ids[side * count + base + i], tiles) for i in range(size)]
            old = [field[row, :] for row in rows]
            new = [old[i] + wide[pl.ds((base + i) * tiles, tiles), :] for i in range(size)]
            if total is not None:
                diagonal = [pot[rows[i], :] * rounded(new[i]) for i in range(size)]
            for i in range(size):
                field[rows[i], :] = new[i]
                if total is not None:
                    total[rows[i], :] = diagonal[i]

        batches(count, BATCH, add)


def rounded(x):
    return x.astype(jnp.bfloat16).astype(jnp.float32)


def slope(bounds, times):
    return (2.0 * times) / jnp.full((1, LANES), bounds[bounds.shape[0] - 1] - bounds[bounds.shape[0] - 2], jnp.float32)


def apply_kernel(step, *refs):
    if step == 0:
        (conn, ids, scales, at, pot_row, stiff_in, start,
         field, total, below, above, pot, stiff, gathered, products, wide) = refs
    else:
        (conn, ids, scales, at, pot, stiff, _, _, came_low, came_high,
         field, total, below, above, gathered, products, wide) = refs
    dofs = stiff.shape[0]
    cells = conn.shape[0] // dofs
    count = ids.shape[0] // 2
    tiles = gathered.shape[0] // dofs
    nodes = field.shape[0] // tiles
    if step == 0:
        stiff[...] = stiff_in[...].T
        width = 512
        for k in range(nodes // width):
            piece = start[:, k * width:(k + 1) * width].astype(jnp.float32)
            node = lax.broadcasted_iota(jnp.int32, piece.shape, 1) + k * width
            turned = jnp.where(node < LN, piece, 0.0).T
            spread = jnp.broadcast_to(pot_row[:, k * width:(k + 1) * width], (LANES, width)).T
            for j in range(tiles):
                rows = pl.ds(k * width * tiles + j, width, tiles)
                value = turned[:, j * LANES:(j + 1) * LANES]
                field[rows, :] = value
                pot[rows, :] = spread
                total[rows, :] = spread * value
    else:
        add_faces(field, (came_low, came_high), wide, ids, slope(scales, min(step, 2)), pot, total)

    def gather(cell, base, size):
        for i in range(size):
            row = conn[cell * dofs + base + i]
            gathered[pl.ds((base + i) * tiles, tiles), :] = field[pl.ds(row, tiles), :]

    def scatter_and_gather(cell, following, base, size):
        rows = [pl.ds(conn[cell * dofs + base + i], tiles) for i in range(size)]
        old = [total[row, :] for row in rows]
        new = [old[i] + products[pl.ds((base + i) * tiles, tiles), :] for i in range(size)]
        for i in range(size):
            total[rows[i], :] = new[i]
        gather(following, base, size)

    batches(dofs, BATCH, functools.partial(gather, 0))

    def one_cell(cell, carry):
        values = jnp.concatenate(
            [gathered[pl.ds(j, dofs, tiles), :].astype(jnp.bfloat16) for j in range(tiles)], axis=1)
        result = jnp.dot(stiff[...], values, preferred_element_type=jnp.float32) * scales[cell]
        for j in range(tiles):
            products[pl.ds(j, dofs, tiles), :] = result[:, j * LANES:(j + 1) * LANES]
        following = jnp.minimum(cell + 1, cells - 1)
        batches(dofs, BATCH, functools.partial(scatter_and_gather, cell, following))
        return carry

    lax.fori_loop(0, cells, one_cell, 0)

    for side, faces in enumerate((below, above)):
        def take(base, size):
            for i in range(size):
                wide[pl.ds((base + i) * tiles, tiles), :] = total[pl.ds(ids[side * count + base + i], tiles), :]

        batches(count, BATCH, take)
        faces[...] = wide[...].astype(faces.dtype)


def settle_kernel(step, last, *refs):
    if step == 0:
        bounds, pot, current, summed, out, total = refs
    else:
        bounds, pot, current, summed, older, out, *total = refs
        total = total[0] if total else None
    center = (bounds[bounds.shape[0] - 1] + bounds[bounds.shape[0] - 2]) * 0.5
    rate = slope(bounds, min(step + 1, 2))

    def some(g, carry):
        rows = pl.ds(pl.multiple_of(g * SPAN, SPAN), SPAN)
        value = rate * (summed[rows, :] - center * rounded(current[rows, :]))
        if step:
            value = value - rounded(older[rows, :])
        out[rows, :] = value
        if not last:
            total[rows, :] = pot[rows, :] * rounded(value)
        return carry

    lax.fori_loop(0, current.shape[0] // SPAN, some, 0)


def node_rows(field, start, width, tiles):
    return jnp.concatenate(
        [field[pl.ds(start * tiles + j, width, tiles), :] for j in range(tiles)], axis=1)


def send_kernel(ids, bounds, at, before, came_low, came_high, field, away, wide):
    count = ids.shape[0] // 2
    tiles = wide.shape[0] // count
    half = away.shape[0]
    add_faces(field, (came_low, came_high), wide, ids, slope(bounds, 2))
    start = (1 - at[0]) * half
    width = WIDTH
    for k in range(half // width):
        away[k * width:(k + 1) * width, :] = node_rows(
            field, start + k * width, width, tiles).astype(away.dtype)


def turn_kernel(ids, at, before, field, turned, own, own_masked, gram):
    count = ids.shape[0] // 2
    states, nodes = turned.shape
    tiles = states // LANES
    half = own.shape[0]
    start = pl.multiple_of(at[0] * half, LANES)
    width = WIDTH
    for k in range(half // width):
        own[k * width:(k + 1) * width, :] = node_rows(
            field, start + k * width, width, tiles).astype(own.dtype)
    for k in range(nodes // width):
        turned[:, k * width:(k + 1) * width] = node_rows(field, k * width, width, tiles).T.astype(turned.dtype)

    @pl.when(at[1] > 0)
    def _():
        def drop(base, size):
            for i in range(size):
                field[pl.ds(ids[base + i], tiles), :] = jnp.zeros((tiles, LANES), jnp.float32)

        batches(count, BATCH, drop)

    for k in range(half // width):
        own_masked[:, k * width:(k + 1) * width] = node_rows(
            field, start + k * width, width, tiles).T.astype(own_masked.dtype)
    total = jnp.zeros(gram.shape, jnp.float32)
    for k in range(nodes // width):
        total += jnp.dot(turned[:, k * width:(k + 1) * width],
                         node_rows(field, k * width, width, tiles).astype(turned.dtype),
                         preferred_element_type=jnp.float32)
    gram[...] = total


def cross_kernel(at, mine, came, out):
    value = jnp.dot(mine[...], came[...], preferred_element_type=jnp.float32)

    @pl.when(at[0] == 0)
    def _():
        out[...] = value

    @pl.when(at[0] != 0)
    def _():
        out[...] = value.T


def split(x):
    high = x.astype(jnp.bfloat16)
    return high, (x - high.astype(jnp.float32)).astype(jnp.bfloat16)


def product(a, b):
    def dot(x, y):
        return jnp.dot(x, y, preferred_element_type=jnp.float32)

    return dot(a[0], b[0]) + (dot(a[0], b[1]) + dot(a[1], b[0]))


def root_kernel(at, blocks, out, gram, held):
    size = blocks.shape[1]
    cross = blocks[2]
    gram[:size, :size] = blocks[0]
    gram[size:, size:] = blocks[1]
    gram[:size, size:] = cross
    gram[size:, :size] = cross.T
    whole = gram[...]
    scale = jnp.sqrt(jnp.sum(whole * whole, keepdims=True) + 1e-06)
    start = pl.multiple_of(at[0] * size, LANES)
    row = lax.broadcasted_iota(jnp.int32, whole.shape, 0)
    column = lax.broadcasted_iota(jnp.int32, whole.shape, 1)
    diagonal = jnp.where(row == column, 1.5, 0.0)
    iterate = whole / scale
    factor = diagonal - 0.5 * iterate
    inverse = None
    for sweep in range(1, NS_ITERS):
        pieces = split(factor)
        iterate = product(split(iterate), split(product(pieces, pieces)))
        factor = diagonal - 0.5 * iterate
        held[0], held[1] = pieces if inverse is None else inverse
        if sweep == NS_ITERS - 1:
            columns = held[0, :, pl.ds(start, size)], held[1, :, pl.ds(start, size)]
            result = product(split(factor), split(product(pieces, columns)))
        else:
            inverse = pieces if inverse is None else split(product(pieces, inverse))
    out[...] = (result / jnp.sqrt(scale)).astype(jnp.bfloat16)


def rotate_kernel(at, columns, turned, first, rest, out):
    states, nodes = out.shape
    half = nodes // 2
    own = columns[pl.ds(pl.multiple_of(at[0] * states, states), states), :]
    other = columns[pl.ds(pl.multiple_of((1 - at[0]) * states, states), states), :]

    def part_of(base, came):
        width = came.shape[0]
        base = pl.multiple_of(base, LANES)
        value = lax.dot_general(
            own, turned[:, pl.ds(base, width)], (((0,), (0,)), ((), ())), preferred_element_type=jnp.float32)
        value += lax.dot_general(
            other, came[...], (((0,), (1,)), ((), ())), preferred_element_type=jnp.float32)
        out[:, pl.ds(base, width)] = value.astype(out.dtype)

    part_of(at[0] * half, first)
    part_of((1 - at[0]) * half, rest)


SMEM = pl.BlockSpec(memory_space=pltpu.SMEM)
VMEM = pl.BlockSpec(memory_space=pltpu.VMEM)
def limit(mib):
    return pltpu.CompilerParams(vmem_limit_bytes=mib * 1024 * 1024)


def struct(shape, dtype=jnp.float32):
    return jax.ShapeDtypeStruct(shape, dtype)


def apply_call(step, tables, pot, stiff, *fields):
    conn, ids = tables[:2]
    dofs = stiff.shape[0]
    count = ids.shape[0] // 2
    f32, bf16 = jnp.float32, jnp.bfloat16
    if step == 0:
        tiles = fields[0].shape[0] // LANES
        rows = fields[0].shape[1] * tiles
    else:
        rows = pot.shape[0]
        tiles = fields[2].shape[0] // count
    face = struct((count * tiles, LANES), bf16)
    whole = struct((rows, LANES))
    out_shape = [whole, whole, face, face]
    if step == 0:
        out_shape += [whole, struct(stiff.shape, stiff.dtype)]
    return pl.pallas_call(
        functools.partial(apply_kernel, step),
        out_shape=out_shape,
        in_specs=[SMEM] * 4 + [VMEM] * (2 + len(fields)),
        out_specs=[VMEM] * len(out_shape),
        scratch_shapes=[
            pltpu.VMEM((dofs * tiles, LANES), f32),
            pltpu.VMEM((dofs * tiles, LANES), f32),
            pltpu.VMEM((count * tiles, LANES), f32),
        ],
        input_output_aliases={6: 0, 7: 1} if step else {},
        compiler_params=limit(26),
        name="apply",
    )(*tables, pot, stiff, *fields)


def settle_call(step, last, bounds, pot, current, total, older=None):
    whole = struct(current.shape)
    fields = [current, total] + ([older] if step else [])
    aliases = {4: 0} if step else {}
    if not last:
        aliases[3] = 1
    return pl.pallas_call(
        functools.partial(settle_kernel, step, last),
        out_shape=[whole] if last else [whole, whole],
        in_specs=[SMEM] + [VMEM] * (1 + len(fields)),
        out_specs=[VMEM] * (1 if last else 2),
        input_output_aliases=aliases,
        compiler_params=limit(26),
        cost_estimate=pl.CostEstimate(flops=8 * 10**9, bytes_accessed=10**7, transcendentals=0),
        name="settle",
    )(bounds, pot, *fields)


def groups_of(devices):
    bits = devices.bit_length() - 1
    return [list(range(b, min(b + 2, bits))) if b else [0] for b in [0] + list(range(1, bits, 2))][:bits]


def plan(group):
    for m in range(1, 1 << len(group)):
        yield m, sum(((m >> i) & 1) << bit for i, bit in enumerate(group))


def code_of(group, here):
    return sum(((here >> bit) & 1) << i for i, bit in enumerate(group))


def sum_scatter(x, here):
    devices = lax.axis_size("dom")
    for group in groups_of(devices):
        size = x.shape[-2] >> len(group)
        code = code_of(group, here)
        came = [
            lax.ppermute(
                lax.dynamic_slice_in_dim(x, (code ^ m) * size, size, x.ndim - 2),
                "dom", [(i, i ^ mask) for i in range(devices)])
            for m, mask in plan(group)
        ]
        x = lax.dynamic_slice_in_dim(x, code * size, size, x.ndim - 2)
        for y in came:
            x = x + y
    return x


def gather_all(x, here):
    devices = lax.axis_size("dom")
    for group in reversed(groups_of(devices)):
        size = x.shape[-2]
        code = code_of(group, here)
        pieces = [(0, x)] + [
            (m, lax.ppermute(x, "dom", [(i, i ^ mask) for i in range(devices)])) for m, mask in plan(group)
        ]
        x = jnp.zeros(x.shape[:-2] + (size << len(group), x.shape[-1]), x.dtype)
        for m, piece in pieces:
            x = lax.dynamic_update_slice_in_dim(x, piece, (code ^ m) * size, x.ndim - 2)
    return x


def rotate_pair(field, away, ids, at, states, nodes):
    f32, bf16 = jnp.float32, jnp.bfloat16
    swap = [(0, 1), (1, 0)]
    half = nodes // 2
    came = lax.ppermute(away, "st", swap)
    _, turned, own, own_masked, gram = pl.pallas_call(
        turn_kernel,
        out_shape=[struct(field.shape), struct((states, nodes), bf16), struct((half, states), bf16),
                   struct((states, half), bf16), struct((states, states))],
        in_specs=[SMEM, SMEM, VMEM], out_specs=[VMEM] * 5,
        input_output_aliases={2: 0},
        compiler_params=limit(26), name="turn",
        cost_estimate=pl.CostEstimate(flops=4 * 10**9, bytes_accessed=10**7, transcendentals=0),
    )(ids, at, field)
    place, gram = lax.optimization_barrier((at, gram))
    here = place[1]
    own_sum = sum_scatter(gram, here)
    cross = pl.pallas_call(
        cross_kernel,
        out_shape=struct((states, states)),
        in_specs=[SMEM, VMEM, VMEM], out_specs=VMEM, compiler_params=limit(16), name="cross",
    )(at, own_masked, came)
    with jax.named_scope("rest"):
        rest = lax.ppermute(own, "st", swap)
    cross_sum = sum_scatter(cross, here)
    pair = jnp.stack([own_sum, cross_sum])
    theirs = lax.ppermute(pair, "st", swap)
    lower = place[0] == 0
    blocks = gather_all(jnp.stack([
        jnp.where(lower, pair[0], theirs[0]), jnp.where(lower, theirs[0], pair[0]), pair[1] + theirs[1]]), here)
    columns = pl.pallas_call(
        root_kernel,
        out_shape=struct((2 * states, states), bf16),
        in_specs=[SMEM, VMEM], out_specs=VMEM,
        scratch_shapes=[pltpu.VMEM((2 * states, 2 * states), f32), pltpu.VMEM((2, 2 * states, 2 * states), bf16)],
        compiler_params=limit(26), name="root",
    )(at, blocks)
    return pl.pallas_call(
        rotate_kernel,
        out_shape=struct((states, nodes), bf16),
        in_specs=[SMEM] + [VMEM] * 4, out_specs=VMEM, compiler_params=limit(26), name="rotate",
    )(at, columns, turned, came, rest)


def rotate_any(current, owned):
    states = current.shape[0]
    whole = lax.all_gather(current, "st", axis=0, tiled=True)
    rows = lax.dot_general(
        current * owned, whole, (((1,), (1,)), ((), ())), preferred_element_type=jnp.float32)
    gram = lax.all_gather(lax.psum(rows, "dom"), "st", axis=0, tiled=True)
    columns = lax.dynamic_slice_in_dim(inverse_root(gram), lax.axis_index("st") * states, states, 1)
    rotated = lax.dot_general(
        columns, whole, (((0,), (0,)), ((), ())), preferred_element_type=jnp.float32)
    return rotated.astype(jnp.bfloat16)


def body(start_states, stiffness, cell_scale, potential, connectivity, shared_nodes, filter_bounds):
    block_states, nodes = start_states.shape
    tiles = pl.cdiv(block_states, LANES)
    states = tiles * LANES
    if states != block_states:
        start_states = jnp.pad(start_states, ((0, states - block_states), (0, 0)))
    conn = connectivity.reshape(-1) * tiles
    ids = shared_nodes.reshape(-1) * tiles
    numbers = jnp.concatenate([cell_scale, filter_bounds])
    at = jnp.stack([lax.axis_index("st"), lax.axis_index("dom")])

    def exchange(low, high):
        with jax.named_scope("halo"):
            return passed_along(high, "dom", 1), passed_along(low, "dom", -1)

    older = None
    current, total, low, high, pot, stiff = apply_call(
        0, (conn, ids, numbers, at), potential[None, :], stiffness, start_states)
    for step in range(DEGREE):
        came = exchange(low, high)
        last = step == DEGREE - 1
        following, *rest = settle_call(step, last, numbers, pot, current, total, older)
        if not last:
            older = current
            current, total, low, high = apply_call(
                step + 1, (conn, ids, numbers, at), pot, stiff, following, rest[0], *came)
            continue
    field, away = pl.pallas_call(
        send_kernel,
        out_shape=[struct(following.shape), struct((nodes // 2, states), jnp.bfloat16)],
        in_specs=[SMEM] * 3 + [VMEM] * 3,
        out_specs=[VMEM] * 2,
        scratch_shapes=[pltpu.VMEM((ids.shape[0] // 2 * tiles, LANES), jnp.float32)],
        input_output_aliases={3: 0},
        compiler_params=limit(26),
        name="send",
    )(ids, numbers, at, following, *came)
    devices = lax.axis_size("dom")
    if lax.axis_size("st") == 2 and states == block_states and devices & (devices - 1) == 0:
        return rotate_pair(field, away, ids, at, states, nodes)
    current = field.reshape(nodes, states).T.astype(jnp.bfloat16)[:block_states]
    inside = (jnp.arange(nodes) < LN).astype(jnp.bfloat16)
    keep = jnp.where(lax.axis_index("dom") > 0, 0.0, 1.0).astype(jnp.bfloat16)
    owned = inside.at[shared_nodes[0, 0]].set(keep)[None, :]
    return rotate_any(current, owned)


def solution(mesh):
    placed = (P("st", "dom"), P(), P("dom"), P("dom"), P("dom", None), P("dom", None, None), P())
    return jax.shard_map(
        body, mesh=mesh, in_specs=placed, out_specs=P("st", "dom"), check_vma=False
    )
```

```python
import functools
import jax
import jax.numpy as jnp
from jax import lax
from jax.experimental import pallas as pl
from jax.experimental.pallas import tpu as pltpu
from jax.sharding import PartitionSpec as P


DEGREE = 3
NS_ITERS = 3
LN = 3480
LANES = 128
BATCH = 16
SPAN = 128
WIDTH = 256


def paired(x, axis, offset):
    devices = lax.axis_size(axis)
    firsts = range(offset, devices - 1, 2)
    pairs = [(i, i + 1) for i in firsts] + [(i + 1, i) for i in firsts]
    return lax.ppermute(x, axis, pairs)


def inverse_root(gram):
    frobenius = jnp.sqrt(jnp.sum(gram * gram) + 1e-06)
    iterate = gram / frobenius
    identity = jnp.eye(gram.shape[0], dtype=jnp.float32)
    inverse = identity
    for _ in range(NS_ITERS):
        factor = 1.5 * identity - 0.5 * jnp.dot(inverse, iterate, precision=lax.Precision.HIGHEST)
        iterate = jnp.dot(iterate, factor, precision=lax.Precision.HIGHEST)
        inverse = jnp.dot(factor, inverse, precision=lax.Precision.HIGHEST)
    return (inverse / jnp.sqrt(frobenius)).astype(jnp.bfloat16)


def batches(count, size, body):
    whole, rest = divmod(count, size)

    def step(g, carry):
        body(pl.multiple_of(g * size, size), size)
        return carry

    lax.fori_loop(0, whole, step, 0)
    if rest:
        body(whole * size, rest)


def add_faces(field, came, wide, ids, at, scale):
    count = ids.shape[0] // 2
    tiles = wide.shape[0] // count
    for slot in range(2):
        wide[...] = came[slot][...].astype(jnp.float32) * scale
        offset = side_of(slot, at) * count

        def add(base, size):
            first = offset + base
            rows = [pl.ds(ids[first + i], tiles) for i in range(size)]
            old = [field[row, :] for row in rows]
            new = [old[i] + wide[pl.ds((base + i) * tiles, tiles), :] for i in range(size)]
            for i in range(size):
                field[rows[i], :] = new[i]

        batches(count, BATCH, add)


def side_of(slot, at):
    odd = at[1] % 2
    return odd if slot else 1 - odd


def rounded(x):
    return x.astype(jnp.bfloat16).astype(jnp.float32)


def slope(bounds, times):
    return (2.0 * times) / jnp.full((1, LANES), bounds[bounds.shape[0] - 1] - bounds[bounds.shape[0] - 2], jnp.float32)


def apply_kernel(step, *refs):
    if step == 0:
        (conn, ids, scales, at, pot_row, stiff_in, start,
         field, total, below, above, pot, stiff, gathered, products, wide) = refs
    else:
        (conn, ids, scales, at, pot, stiff, _, _, came_low, came_high,
         field, total, below, above, gathered, products, wide) = refs
    dofs = stiff.shape[0]
    cells = conn.shape[0] // dofs
    count = ids.shape[0] // 2
    tiles = gathered.shape[0] // dofs
    nodes = field.shape[0] // tiles
    if step == 0:
        width = 512
        pieces = nodes // width
        for k in range(pieces):
            spread = jnp.broadcast_to(pot_row[k * width:(k + 1) * width].reshape(1, width), (LANES, width)).T
            piece = start[:, k * width:(k + 1) * width].astype(jnp.float32)
            node = lax.broadcasted_iota(jnp.int32, piece.shape, 1) + k * width
            turned = jnp.where(node < LN, piece, 0.0).T
            for j in range(tiles):
                rows = pl.ds(k * width * tiles + j, width, tiles)
                field[rows, :] = turned[:, j * LANES:(j + 1) * LANES]
                pot[rows, :] = spread
                total[rows, :] = jnp.zeros_like(spread)
        stiff[...] = stiff_in[...].T
    else:
        add_faces(field, (came_low, came_high), wide, ids, at, slope(scales, min(step, 2)))

    def gather(cell, base, size):
        for i in range(size):
            row = conn[cell * dofs + base + i]
            gathered[pl.ds((base + i) * tiles, tiles), :] = field[pl.ds(row, tiles), :]

    def scatter_and_gather(cell, following, base, size):
        rows = [pl.ds(conn[cell * dofs + base + i], tiles) for i in range(size)]
        old = [total[row, :] for row in rows]
        new = [old[i] + products[pl.ds((base + i) * tiles, tiles), :] for i in range(size)]
        for i in range(size):
            total[rows[i], :] = new[i]
        gather(following, base, size)

    batches(dofs, BATCH, functools.partial(gather, 0))

    def one_cell(cell, carry):
        values = jnp.concatenate(
            [gathered[pl.ds(j, dofs, tiles), :].astype(jnp.bfloat16) for j in range(tiles)], axis=1)
        result = jnp.dot(stiff[...], values, preferred_element_type=jnp.float32) * scales[cell]
        for j in range(tiles):
            products[pl.ds(j, dofs, tiles), :] = result[:, j * LANES:(j + 1) * LANES]
        following = jnp.minimum(cell + 1, cells - 1)
        batches(dofs, BATCH, functools.partial(scatter_and_gather, cell, following))
        return carry

    lax.fori_loop(0, cells, one_cell, 0)

    for slot, faces in enumerate((below, above)):
        offset = side_of(slot, at) * count

        def take(base, size):
            first = offset + base
            for i in range(size):
                row = pl.ds(ids[first + i], tiles)
                wide[pl.ds((base + i) * tiles, tiles), :] = total[row, :] + pot[row, :] * rounded(field[row, :])

        batches(count, BATCH, take)
        faces[...] = wide[...].astype(faces.dtype)


def settle_kernel(step, last, *refs):
    if step == 0:
        bounds, pot, current, summed, out, total = refs
    else:
        bounds, pot, current, summed, older, out, *total = refs
        total = total[0] if total else None
    center = (bounds[bounds.shape[0] - 1] + bounds[bounds.shape[0] - 2]) * 0.5
    rate = slope(bounds, min(step + 1, 2))

    def some(g, carry):
        rows = pl.ds(pl.multiple_of(g * SPAN, SPAN), SPAN)
        value = rate * (summed[rows, :] + (pot[rows, :] - center) * rounded(current[rows, :]))
        if step:
            value = value - rounded(older[rows, :])
        out[rows, :] = value
        if not last:
            total[rows, :] = jnp.zeros_like(value)
        return carry

    lax.fori_loop(0, current.shape[0] // SPAN, some, 0)


def node_rows(field, start, width, tiles):
    return jnp.concatenate(
        [field[pl.ds(start * tiles + j, width, tiles), :] for j in range(tiles)], axis=1)


def send_kernel(ids, bounds, at, before, came_low, came_high, field, away, wide):
    count = ids.shape[0] // 2
    tiles = wide.shape[0] // count
    half = away.shape[0]
    add_faces(field, (came_low, came_high), wide, ids, at, slope(bounds, 2))
    start = (1 - at[0]) * half
    width = WIDTH
    for k in range(half // width):
        away[k * width:(k + 1) * width, :] = node_rows(
            field, start + k * width, width, tiles).astype(away.dtype)


def turn_kernel(ids, at, before, field, turned, own_first, own_second, own_masked, gram):
    count = ids.shape[0] // 2
    states, nodes = turned.shape
    tiles = states // LANES
    quarter = own_first.shape[0]
    half = 2 * quarter
    start = pl.multiple_of(at[0] * half, LANES)
    for k, own in enumerate((own_first, own_second)):
        own[...] = node_rows(field, start + k * quarter, quarter, tiles).astype(own.dtype)
    width = WIDTH
    for k in range(nodes // width):
        turned[:, k * width:(k + 1) * width] = node_rows(field, k * width, width, tiles).T.astype(turned.dtype)

    @pl.when(at[1] > 0)
    def _():
        def drop(base, size):
            for i in range(size):
                field[pl.ds(ids[base + i], tiles), :] = jnp.zeros((tiles, LANES), jnp.float32)

        batches(count, BATCH, drop)

    for k in range(half // width):
        own_masked[:, k * width:(k + 1) * width] = node_rows(
            field, start + k * width, width, tiles).T.astype(own_masked.dtype)
    total = jnp.zeros((states, states), jnp.float32)
    for k in range(nodes // width):
        total += jnp.dot(turned[:, k * width:(k + 1) * width],
                         node_rows(field, k * width, width, tiles).astype(turned.dtype),
                         preferred_element_type=jnp.float32)
    gram[...] = total


def cross_kernel(at, mine, came, out):
    value = jnp.dot(mine[...], came[...], preferred_element_type=jnp.float32)

    @pl.when(at[0] == 0)
    def _():
        out[...] = value

    @pl.when(at[0] != 0)
    def _():
        out[...] = value.T


def split(x):
    high = x.astype(jnp.bfloat16)
    return high, (x - high.astype(jnp.float32)).astype(jnp.bfloat16)


def product(a, b):
    def dot(x, y):
        return jnp.dot(x, y, preferred_element_type=jnp.float32)

    return dot(a[0], b[0]) + (dot(a[0], b[1]) + dot(a[1], b[0]))


def root_kernel(at, blocks, out, gram, held):
    size = blocks.shape[1]
    cross = blocks[2]
    gram[:size, :size] = blocks[0]
    gram[size:, size:] = blocks[1]
    gram[:size, size:] = cross
    gram[size:, :size] = cross.T
    whole = gram[...]
    scale = jnp.sqrt(jnp.sum(whole * whole, keepdims=True) + 1e-06)
    start = pl.multiple_of(at[0] * size, LANES)
    row = lax.broadcasted_iota(jnp.int32, whole.shape, 0)
    column = lax.broadcasted_iota(jnp.int32, whole.shape, 1)
    diagonal = jnp.where(row == column, 1.5, 0.0)
    iterate = whole / scale
    factor = diagonal - 0.5 * iterate
    inverse = None
    for sweep in range(1, NS_ITERS):
        pieces = split(factor)
        iterate = product(split(iterate), split(product(pieces, pieces)))
        factor = diagonal - 0.5 * iterate
        held[0], held[1] = pieces if inverse is None else inverse
        if sweep == NS_ITERS - 1:
            columns = held[0, :, pl.ds(start, size)], held[1, :, pl.ds(start, size)]
            result = product(split(factor), split(product(pieces, columns)))
        else:
            inverse = pieces if inverse is None else split(product(pieces, inverse))
    out[...] = (result / jnp.sqrt(scale)).astype(jnp.bfloat16)


def rotate_kernel(at, columns, turned, first, rest_first, rest_second, out):
    states, nodes = out.shape
    half = nodes // 2
    own = columns[pl.ds(pl.multiple_of(at[0] * states, states), states), :]
    other = columns[pl.ds(pl.multiple_of((1 - at[0]) * states, states), states), :]

    def part_of(base, came):
        width = came.shape[0]
        base = pl.multiple_of(base, LANES)
        value = lax.dot_general(
            own, turned[:, pl.ds(base, width)], (((0,), (0,)), ((), ())), preferred_element_type=jnp.float32)
        value += lax.dot_general(
            other, came[...], (((0,), (1,)), ((), ())), preferred_element_type=jnp.float32)
        out[:, pl.ds(base, width)] = value.astype(out.dtype)

    part_of(at[0] * half, first)
    away = (1 - at[0]) * half
    part_of(away, rest_first)
    part_of(away + rest_first.shape[0], rest_second)


def rotate_call(at, columns, turned, *came):
    return pl.pallas_call(
        rotate_kernel,
        out_shape=struct(turned.shape, jnp.bfloat16),
        in_specs=[SMEM] + [VMEM] * 5, out_specs=VMEM, compiler_params=limit(26), name="rotate",
    )(at, columns, turned, *came)


SMEM = pl.BlockSpec(memory_space=pltpu.SMEM)
VMEM = pl.BlockSpec(memory_space=pltpu.VMEM)


def limit(mib):
    return pltpu.CompilerParams(vmem_limit_bytes=mib * 1024 * 1024)


def struct(shape, dtype=jnp.float32):
    return jax.ShapeDtypeStruct(shape, dtype)


def apply_call(step, tables, pot, stiff, *fields):
    _, ids = tables[:2]
    dofs = stiff.shape[0]
    count = ids.shape[0] // 2
    f32, bf16 = jnp.float32, jnp.bfloat16
    if step == 0:
        tiles = fields[0].shape[0] // LANES
        rows = fields[0].shape[1] * tiles
    else:
        rows = pot.shape[0]
        tiles = fields[2].shape[0] // count
    face = struct((count * tiles, LANES), bf16)
    whole = struct((rows, LANES))
    out_shape = [whole, whole, face, face]
    if step == 0:
        out_shape += [whole, struct(stiff.shape, stiff.dtype)]
    scratch = [
        pltpu.VMEM((dofs * tiles, LANES), f32),
        pltpu.VMEM((dofs * tiles, LANES), f32),
        pltpu.VMEM((count * tiles, LANES), f32),
    ]
    specs = [VMEM] * (2 + len(fields))
    return pl.pallas_call(
        functools.partial(apply_kernel, step),
        out_shape=out_shape,
        in_specs=[SMEM] * 4 + specs,
        out_specs=[VMEM] * len(out_shape),
        scratch_shapes=scratch,
        input_output_aliases={6: 0, 7: 1} if step else {},
        compiler_params=limit(26),
        name="apply",
    )(*tables, pot, stiff, *fields)


def settle_call(step, last, bounds, pot, current, total, older=None):
    whole = struct(current.shape)
    fields = [current, total] + ([older] if step else [])
    aliases = {4: 0} if step else {}
    if not last:
        aliases[3] = 1
    return pl.pallas_call(
        functools.partial(settle_kernel, step, last),
        out_shape=[whole] if last else [whole, whole],
        in_specs=[SMEM] + [VMEM] * (1 + len(fields)),
        out_specs=[VMEM] * (1 if last else 2),
        input_output_aliases=aliases,
        compiler_params=limit(26),
        cost_estimate=pl.CostEstimate(flops=8 * 10**9, bytes_accessed=10**7, transcendentals=0),
        name="settle",
    )(bounds, pot, *fields)


def groups_of(devices):
    bits = devices.bit_length() - 1
    return [list(range(b, min(b + 2, bits))) if b else [0] for b in [0] + list(range(1, bits, 2))][:bits]


def plan(group):
    for m in range(1, 1 << len(group)):
        yield m, sum(((m >> i) & 1) << bit for i, bit in enumerate(group))


def code_of(group, here):
    return sum(((here >> bit) & 1) << i for i, bit in enumerate(group))


def sum_scatter(x, here):
    devices = lax.axis_size("dom")
    for group in groups_of(devices)[:-1]:
        size = x.shape[-2] >> len(group)
        code = code_of(group, here)
        came = [
            lax.ppermute(
                lax.dynamic_slice_in_dim(x, (code ^ m) * size, size, x.ndim - 2),
                "dom", [(i, i ^ mask) for i in range(devices)])
            for m, mask in plan(group)
        ]
        x = lax.dynamic_slice_in_dim(x, code * size, size, x.ndim - 2)
        for y in came:
            x = x + y
    return x


def sum_last(own, cross, part):
    devices = lax.axis_size("dom")
    both = jnp.stack([own, cross])
    sums = []
    for flip in range(2):
        total = None
        for m, mask in [(0, 0)] + list(plan(groups_of(devices)[-1])):
            piece = both
            if mask or flip:
                piece = lax.ppermute(both, ("dom", "st"), [(i, i ^ (2 * mask + flip)) for i in range(2 * devices)])
            total = piece if total is None else total + piece
        sums.append(total)
    mine, theirs = sums
    return jnp.stack([jnp.where(part == 0, mine[0], theirs[0]),
                      jnp.where(part == 0, theirs[0], mine[0]), mine[1] + theirs[1]])


def gather_all(x, here):
    devices = lax.axis_size("dom")
    for group in reversed(groups_of(devices)[:-1]):
        size = x.shape[-2]
        code = code_of(group, here)
        pieces = [(0, x)] + [
            (m, lax.ppermute(x, "dom", [(i, i ^ mask) for i in range(devices)])) for m, mask in plan(group)
        ]
        x = jnp.zeros(x.shape[:-2] + (size << len(group), x.shape[-1]), x.dtype)
        for m, piece in pieces:
            x = lax.dynamic_update_slice_in_dim(x, piece, (code ^ m) * size, x.ndim - 2)
    return x


def rotate_pair(field, away, ids, at, states, nodes):
    f32, bf16 = jnp.float32, jnp.bfloat16
    swap = [(0, 1), (1, 0)]
    half = nodes // 2
    square = struct((states, states))
    came = lax.ppermute(away, "st", swap)
    _, turned, own_first, own_second, own_masked, gram = pl.pallas_call(
        turn_kernel,
        out_shape=[struct(field.shape), struct((states, nodes), bf16),
                   struct((half // 2, states), bf16), struct((half // 2, states), bf16),
                   struct((states, half), bf16), square],
        in_specs=[SMEM, SMEM, VMEM], out_specs=[VMEM] * 6,
        input_output_aliases={2: 0},
        compiler_params=limit(26), name="turn",
        cost_estimate=pl.CostEstimate(flops=4 * 10**9, bytes_accessed=10**7, transcendentals=0),
    )(ids, at, field)
    place, gram = lax.optimization_barrier((at, gram))
    here = place[1]
    own_sum = sum_scatter(gram, here)
    own_masked, own_sum = lax.optimization_barrier((own_masked, own_sum))
    cross = pl.pallas_call(
        cross_kernel,
        out_shape=square,
        in_specs=[SMEM, VMEM, VMEM], out_specs=VMEM, compiler_params=limit(16), name="cross",
    )(at, own_masked, came)
    rest_first = lax.ppermute(own_first, "st", swap)
    cross_sum = sum_scatter(cross, here)
    sums = sum_last(own_sum, cross_sum, place[0])
    rest_second = lax.ppermute(own_second, "st", swap)
    blocks = gather_all(sums, here)
    columns = pl.pallas_call(
        root_kernel,
        out_shape=struct((2 * states, states), bf16),
        in_specs=[SMEM, VMEM], out_specs=VMEM,
        scratch_shapes=[pltpu.VMEM((2 * states, 2 * states), f32), pltpu.VMEM((2, 2 * states, 2 * states), bf16)],
        compiler_params=limit(26), name="root",
    )(at, blocks)
    return rotate_call(at, columns, turned, came, rest_first, rest_second)


def rotate_any(current, owned):
    states = current.shape[0]
    whole = lax.all_gather(current, "st", axis=0, tiled=True)
    rows = lax.dot_general(
        current * owned, whole, (((1,), (1,)), ((), ())), preferred_element_type=jnp.float32)
    gram = lax.all_gather(lax.psum(rows, "dom"), "st", axis=0, tiled=True)
    columns = lax.dynamic_slice_in_dim(inverse_root(gram), lax.axis_index("st") * states, states, 1)
    rotated = lax.dot_general(
        columns, whole, (((0,), (0,)), ((), ())), preferred_element_type=jnp.float32)
    return rotated.astype(jnp.bfloat16)


def body(start_states, stiffness, cell_scale, potential, connectivity, shared_nodes, filter_bounds):
    block_states, nodes = start_states.shape
    tiles = pl.cdiv(block_states, LANES)
    states = tiles * LANES
    if states != block_states:
        start_states = jnp.pad(start_states, ((0, states - block_states), (0, 0)))
    conn = connectivity.reshape(-1) * tiles
    ids = shared_nodes.reshape(-1) * tiles
    numbers = jnp.concatenate([cell_scale, filter_bounds])
    at = jnp.stack([lax.axis_index("st"), lax.axis_index("dom")])

    def exchange(low, high):
        return paired(low, "dom", 0), paired(high, "dom", 1)

    older = None
    current, total, low, high, pot, stiff = apply_call(
        0, (conn, ids, numbers, at), potential, stiffness, start_states)
    for step in range(DEGREE):
        came = exchange(low, high)
        last = step == DEGREE - 1
        following, *rest = settle_call(step, last, numbers, pot, current, total, older)
        if not last:
            older = current
            current, total, low, high = apply_call(
                step + 1, (conn, ids, numbers, at), pot, stiff, following, rest[0], *came)
            continue
    field, away = pl.pallas_call(
        send_kernel,
        out_shape=[struct(following.shape), struct((nodes // 2, states), jnp.bfloat16)],
        in_specs=[SMEM] * 3 + [VMEM] * 3,
        out_specs=[VMEM] * 2,
        scratch_shapes=[pltpu.VMEM((ids.shape[0] // 2 * tiles, LANES), jnp.float32)],
        input_output_aliases={3: 0},
        compiler_params=limit(26),
        name="send",
    )(ids, numbers, at, following, *came)
    devices = lax.axis_size("dom")
    if lax.axis_size("st") == 2 and states == block_states and devices & (devices - 1) == nodes % (4 * LANES):
        return rotate_pair(field, away, ids, at, states, nodes)
    current = field.reshape(nodes, states).T.astype(jnp.bfloat16)[:block_states]
    inside = (jnp.arange(nodes) < LN).astype(jnp.bfloat16)
    keep = jnp.where(lax.axis_index("dom") > 0, 0.0, 1.0).astype(jnp.bfloat16)
    owned = inside.at[shared_nodes[0, 0]].set(keep)[None, :]
    return rotate_any(current, owned)


def solution(mesh):
    placed = (P("st", "dom"), P(), P("dom"), P("dom"), P("dom", None), P("dom", None, None), P())
    return jax.shard_map(body, mesh=mesh, in_specs=placed, out_specs=P("st", "dom"), check_vma=False)
```

```python
import functools
import jax
import jax.numpy as jnp
from jax import lax
from jax.experimental import pallas as pl
from jax.experimental.pallas import tpu as pltpu
from jax.sharding import PartitionSpec as P


DEGREE = 3
NS_ITERS = 3
LN = 3480
LANES = 128
BATCH = 16
GROUP = 2
SPAN = 128
WIDTH = 256


def paired(x, axis, offset):
    devices = lax.axis_size(axis)
    firsts = range(offset, devices - 1, 2)
    pairs = [(i, i + 1) for i in firsts] + [(i + 1, i) for i in firsts]
    return lax.ppermute(x, axis, pairs)


def inverse_root(gram):
    frobenius = jnp.sqrt(jnp.sum(gram * gram) + 1e-06)
    iterate = gram / frobenius
    identity = jnp.eye(gram.shape[0], dtype=jnp.float32)
    inverse = identity
    for _ in range(NS_ITERS):
        factor = 1.5 * identity - 0.5 * jnp.dot(inverse, iterate, precision=lax.Precision.HIGHEST)
        iterate = jnp.dot(iterate, factor, precision=lax.Precision.HIGHEST)
        inverse = jnp.dot(factor, inverse, precision=lax.Precision.HIGHEST)
    return (inverse / jnp.sqrt(frobenius)).astype(jnp.bfloat16)


def batches(count, size, body):
    whole, rest = divmod(count, size)

    def step(g, carry):
        body(pl.multiple_of(g * size, size), size)
        return carry

    lax.fori_loop(0, whole, step, 0)
    if rest:
        body(whole * size, rest)


def add_faces(field, came, wide, ids, at, scale):
    count = ids.shape[0] // 2
    tiles = wide.shape[0] // count
    for slot in range(2):
        wide[...] = came[slot][...].astype(jnp.float32) * scale
        offset = side_of(slot, at) * count

        def add(base, size):
            first = offset + base
            rows = [pl.ds(ids[first + i], tiles) for i in range(size)]
            old = [field[row, :] for row in rows]
            new = [old[i] + wide[pl.ds((base + i) * tiles, tiles), :] for i in range(size)]
            for i in range(size):
                field[rows[i], :] = new[i]

        batches(count, BATCH, add)


def side_of(slot, at):
    odd = at[1] % 2
    return odd if slot else 1 - odd


def rounded(x):
    return x.astype(jnp.bfloat16).astype(jnp.float32)


def slope(bounds, times):
    return (2.0 * times) / jnp.full((1, LANES), bounds[bounds.shape[0] - 1] - bounds[bounds.shape[0] - 2], jnp.float32)


def apply_kernel(step, *refs):
    if step == 0:
        (conn, ids, scales, at, pot_row, stiff_in, start,
         field, total, below, above, pot, stiff, gathered, products, wide) = refs
    else:
        (conn, ids, scales, at, pot, stiff, _, _, came_low, came_high,
         field, total, below, above, gathered, products, wide) = refs
    dofs = stiff.shape[0]
    cells = conn.shape[0] * LANES // dofs
    count = ids.shape[0] // 2
    tiles = gathered.shape[0] // (GROUP * dofs)
    nodes = field.shape[0] // tiles
    if step == 0:
        width = 512
        pieces = nodes // width
        for k in range(pieces):
            spread = jnp.broadcast_to(pot_row[k * width:(k + 1) * width].reshape(1, width), (LANES, width)).T
            piece = start[:, k * width:(k + 1) * width].astype(jnp.float32)
            node = lax.broadcasted_iota(jnp.int32, piece.shape, 1) + k * width
            turned = jnp.where(node < LN, piece, 0.0).T
            for j in range(tiles):
                rows = pl.ds(k * width * tiles + j, width, tiles)
                field[rows, :] = turned[:, j * LANES:(j + 1) * LANES]
                pot[rows, :] = spread
                total[rows, :] = jnp.zeros_like(spread)
        stiff[...] = stiff_in[...].T
    else:
        add_faces(field, (came_low, came_high), wide, ids, at, slope(scales, min(step, 2)))

    lines = conn.shape[0] // cells * GROUP

    def gather(line, base):
        for i in range(BATCH):
            gathered[pl.ds((line % lines * LANES + base + i) * tiles, tiles), :] = field[
                pl.ds(conn[line, base + i], tiles), :]

    def gather_line(line):
        for base in range(0, LANES, BATCH):
            gather(line, base)

    def scatter_line(line, following):
        for base in range(0, LANES, BATCH):
            rows = [pl.ds(conn[line, base + i], tiles) for i in range(BATCH)]
            old = [total[row, :] for row in rows]
            first = (line % lines * LANES + base) * tiles
            new = [old[i] + products[pl.ds(first + i * tiles, tiles), :] for i in range(BATCH)]
            for i in range(BATCH):
                total[rows[i], :] = new[i]
            gather(following, base)

    def begin(line, carry):
        gather_line(line)
        return carry

    lax.fori_loop(0, lines, begin, 0)

    def some_cells(group, carry):
        values = jnp.concatenate(
            [gathered[pl.ds(c * dofs * tiles + j, dofs, tiles), :].astype(jnp.bfloat16)
             for c in range(GROUP) for j in range(tiles)], axis=1)
        result = jnp.dot(stiff[...], values, preferred_element_type=jnp.float32)
        for c in range(GROUP):
            scale = scales[group * GROUP + c]
            for j in range(tiles):
                at_lane = (c * tiles + j) * LANES
                products[pl.ds(c * dofs * tiles + j, dofs, tiles), :] = result[:, at_lane:at_lane + LANES] * scale
        following = jnp.minimum(group + 1, cells // GROUP - 1)

        def some(r, carried):
            scatter_line(group * lines + r, following * lines + r)
            return carried

        lax.fori_loop(0, lines, some, 0)
        return carry

    lax.fori_loop(0, cells // GROUP, some_cells, 0)

    for slot, faces in enumerate((below, above)):
        offset = side_of(slot, at) * count

        def take(base, size):
            first = offset + base
            for i in range(size):
                row = pl.ds(ids[first + i], tiles)
                wide[pl.ds((base + i) * tiles, tiles), :] = total[row, :] + pot[row, :] * rounded(field[row, :])

        batches(count, BATCH, take)
        faces[...] = wide[...].astype(faces.dtype)


def settle_kernel(step, last, *refs):
    if step == 0:
        bounds, pot, current, summed, out, total = refs
    else:
        bounds, pot, current, summed, older, out, *total = refs
        total = total[0] if total else None
    center = (bounds[bounds.shape[0] - 1] + bounds[bounds.shape[0] - 2]) * 0.5
    rate = slope(bounds, min(step + 1, 2))

    def some(g, carry):
        rows = pl.ds(pl.multiple_of(g * SPAN, SPAN), SPAN)
        value = rate * (summed[rows, :] + (pot[rows, :] - center) * rounded(current[rows, :]))
        if step:
            value = value - rounded(older[rows, :])
        out[rows, :] = value
        if not last:
            total[rows, :] = jnp.zeros_like(value)
        return carry

    lax.fori_loop(0, current.shape[0] // SPAN, some, 0)


def node_rows(field, start, width, tiles):
    return jnp.concatenate(
        [field[pl.ds(start * tiles + j, width, tiles), :] for j in range(tiles)], axis=1)


def send_kernel(ids, bounds, at, before, came_low, came_high, field, away, wide):
    count = ids.shape[0] // 2
    tiles = wide.shape[0] // count
    half = away.shape[0]
    add_faces(field, (came_low, came_high), wide, ids, at, slope(bounds, 2))
    start = (1 - at[0]) * half
    width = WIDTH
    for k in range(half // width):
        away[k * width:(k + 1) * width, :] = node_rows(
            field, start + k * width, width, tiles).astype(away.dtype)


def turn_kernel(ids, at, before, field, turned, own, own_masked, gram):
    count = ids.shape[0] // 2
    states, nodes = turned.shape
    tiles = states // LANES
    half = own.shape[0]
    start = pl.multiple_of(at[0] * half, LANES)
    width = WIDTH
    for k in range(half // width):
        own[k * width:(k + 1) * width, :] = node_rows(
            field, start + k * width, width, tiles).astype(own.dtype)
    for k in range(nodes // width):
        turned[:, k * width:(k + 1) * width] = node_rows(field, k * width, width, tiles).T.astype(turned.dtype)

    @pl.when(at[1] > 0)
    def _():
        def drop(base, size):
            for i in range(size):
                field[pl.ds(ids[base + i], tiles), :] = jnp.zeros((tiles, LANES), jnp.float32)

        batches(count, BATCH, drop)

    for k in range(half // width):
        own_masked[:, k * width:(k + 1) * width] = node_rows(
            field, start + k * width, width, tiles).T.astype(own_masked.dtype)
    total = jnp.zeros((states, states), jnp.float32)
    for k in range(nodes // width):
        total += jnp.dot(turned[:, k * width:(k + 1) * width],
                         node_rows(field, k * width, width, tiles).astype(turned.dtype),
                         preferred_element_type=jnp.float32)
    gram[...] = total


def cross_kernel(at, mine, came, out):
    value = jnp.dot(mine[...], came[...], preferred_element_type=jnp.float32)

    @pl.when(at[0] == 0)
    def _():
        out[...] = value

    @pl.when(at[0] != 0)
    def _():
        out[...] = value.T


def split(x):
    high = x.astype(jnp.bfloat16)
    return high, (x - high.astype(jnp.float32)).astype(jnp.bfloat16)


def product(a, b):
    def dot(x, y):
        return jnp.dot(x, y, preferred_element_type=jnp.float32)

    return dot(a[0], b[0]) + (dot(a[0], b[1]) + dot(a[1], b[0]))


def root_kernel(at, blocks, out, gram, held):
    size = blocks.shape[1]
    cross = blocks[2]
    gram[:size, :size] = blocks[0]
    gram[size:, size:] = blocks[1]
    gram[:size, size:] = cross
    gram[size:, :size] = cross.T
    whole = gram[...]
    scale = jnp.sqrt(jnp.sum(whole * whole, keepdims=True) + 1e-06)
    start = pl.multiple_of(at[0] * size, LANES)
    row = lax.broadcasted_iota(jnp.int32, whole.shape, 0)
    column = lax.broadcasted_iota(jnp.int32, whole.shape, 1)
    diagonal = jnp.where(row == column, 1.5, 0.0)
    iterate = whole / scale
    factor = diagonal - 0.5 * iterate
    inverse = None
    for sweep in range(1, NS_ITERS):
        pieces = split(factor)
        iterate = product(split(iterate), split(product(pieces, pieces)))
        factor = diagonal - 0.5 * iterate
        held[0], held[1] = pieces if inverse is None else inverse
        if sweep == NS_ITERS - 1:
            columns = held[0, :, pl.ds(start, size)], held[1, :, pl.ds(start, size)]
            result = product(split(factor), split(product(pieces, columns)))
        else:
            inverse = pieces if inverse is None else split(product(pieces, inverse))
    out[...] = (result / jnp.sqrt(scale)).astype(jnp.bfloat16)


def rotate_kernel(at, columns, turned, first, rest, out):
    states, nodes = out.shape
    half = nodes // 2
    own = columns[pl.ds(pl.multiple_of(at[0] * states, states), states), :]
    other = columns[pl.ds(pl.multiple_of((1 - at[0]) * states, states), states), :]

    def part_of(base, came):
        width = came.shape[0]
        base = pl.multiple_of(base, LANES)
        value = lax.dot_general(
            own, turned[:, pl.ds(base, width)], (((0,), (0,)), ((), ())), preferred_element_type=jnp.float32)
        value += lax.dot_general(
            other, came[...], (((0,), (1,)), ((), ())), preferred_element_type=jnp.float32)
        out[:, pl.ds(base, width)] = value.astype(out.dtype)

    part_of(at[0] * half, first)
    part_of((1 - at[0]) * half, rest)


def rotate_call(at, columns, turned, *came):
    return pl.pallas_call(
        rotate_kernel,
        out_shape=struct(turned.shape, jnp.bfloat16),
        in_specs=[SMEM] + [VMEM] * 4, out_specs=VMEM, compiler_params=limit(26), name="rotate",
    )(at, columns, turned, *came)


SMEM = pl.BlockSpec(memory_space=pltpu.SMEM)
VMEM = pl.BlockSpec(memory_space=pltpu.VMEM)


def limit(mib):
    return pltpu.CompilerParams(vmem_limit_bytes=mib * 1024 * 1024)


def struct(shape, dtype=jnp.float32):
    return jax.ShapeDtypeStruct(shape, dtype)


def apply_call(step, tables, pot, stiff, *fields):
    _, ids = tables[:2]
    dofs = stiff.shape[0]
    count = ids.shape[0] // 2
    f32, bf16 = jnp.float32, jnp.bfloat16
    if step == 0:
        tiles = fields[0].shape[0] // LANES
        rows = fields[0].shape[1] * tiles
    else:
        rows = pot.shape[0]
        tiles = fields[2].shape[0] // count
    face = struct((count * tiles, LANES), bf16)
    whole = struct((rows, LANES))
    out_shape = [whole, whole, face, face]
    if step == 0:
        out_shape += [whole, struct(stiff.shape, stiff.dtype)]
    scratch = [
        pltpu.VMEM((GROUP * dofs * tiles, LANES), f32),
        pltpu.VMEM((GROUP * dofs * tiles, LANES), f32),
        pltpu.VMEM((count * tiles, LANES), f32),
    ]
    specs = [VMEM] * (2 + len(fields))
    return pl.pallas_call(
        functools.partial(apply_kernel, step),
        out_shape=out_shape,
        in_specs=[SMEM] * 4 + specs,
        out_specs=[VMEM] * len(out_shape),
        scratch_shapes=scratch,
        input_output_aliases={6: 0, 7: 1} if step else {},
        compiler_params=limit(26),
        name="apply",
    )(*tables, pot, stiff, *fields)


def settle_call(step, last, bounds, pot, current, total, older=None):
    whole = struct(current.shape)
    fields = [current, total] + ([older] if step else [])
    aliases = {4: 0} if step else {}
    if not last:
        aliases[3] = 1
    return pl.pallas_call(
        functools.partial(settle_kernel, step, last),
        out_shape=[whole] if last else [whole, whole],
        in_specs=[SMEM] + [VMEM] * (1 + len(fields)),
        out_specs=[VMEM] * (1 if last else 2),
        input_output_aliases=aliases,
        compiler_params=limit(26),
        cost_estimate=pl.CostEstimate(flops=8 * 10**9, bytes_accessed=10**7, transcendentals=0),
        name="settle",
    )(bounds, pot, *fields)


def groups_of(devices):
    bits = devices.bit_length() - 1
    return [list(range(b, min(b + 2, bits))) if b else [0] for b in [0] + list(range(1, bits, 2))][:bits]


def plan(group):
    for m in range(1, 1 << len(group)):
        yield m, sum(((m >> i) & 1) << bit for i, bit in enumerate(group))


def code_of(group, here):
    return sum(((here >> bit) & 1) << i for i, bit in enumerate(group))


def sum_scatter(x, here):
    devices = lax.axis_size("dom")
    for group in groups_of(devices)[:-1]:
        size = x.shape[-2] >> len(group)
        code = code_of(group, here)
        came = [
            lax.ppermute(
                lax.dynamic_slice_in_dim(x, (code ^ m) * size, size, x.ndim - 2),
                "dom", [(i, i ^ mask) for i in range(devices)])
            for m, mask in plan(group)
        ]
        x = lax.dynamic_slice_in_dim(x, code * size, size, x.ndim - 2)
        for y in came:
            x = x + y
    return x


def sum_last(own, cross, part):
    devices = lax.axis_size("dom")
    both = jnp.stack([own, cross])
    sums = []
    for flip in range(2):
        total = None
        for m, mask in [(0, 0)] + list(plan(groups_of(devices)[-1])):
            piece = both
            if mask or flip:
                piece = lax.ppermute(both, ("dom", "st"), [(i, i ^ (2 * mask + flip)) for i in range(2 * devices)])
            total = piece if total is None else total + piece
        sums.append(total)
    mine, theirs = sums
    return jnp.stack([jnp.where(part == 0, mine[0], theirs[0]),
                      jnp.where(part == 0, theirs[0], mine[0]), mine[1] + theirs[1]])


def gather_all(x, here):
    devices = lax.axis_size("dom")
    for group in reversed(groups_of(devices)[:-1]):
        size = x.shape[-2]
        code = code_of(group, here)
        pieces = [(0, x)] + [
            (m, lax.ppermute(x, "dom", [(i, i ^ mask) for i in range(devices)])) for m, mask in plan(group)
        ]
        x = jnp.zeros(x.shape[:-2] + (size << len(group), x.shape[-1]), x.dtype)
        for m, piece in pieces:
            x = lax.dynamic_update_slice_in_dim(x, piece, (code ^ m) * size, x.ndim - 2)
    return x


def rotate_pair(field, away, ids, at, states, nodes):
    f32, bf16 = jnp.float32, jnp.bfloat16
    swap = [(0, 1), (1, 0)]
    half = nodes // 2
    square = struct((states, states))
    came = lax.ppermute(away, "st", swap)
    _, turned, own, own_masked, gram = pl.pallas_call(
        turn_kernel,
        out_shape=[struct(field.shape), struct((states, nodes), bf16),
                   struct((half, states), bf16),
                   struct((states, half), bf16), square],
        in_specs=[SMEM, SMEM, VMEM], out_specs=[VMEM] * 5,
        input_output_aliases={2: 0},
        compiler_params=limit(26), name="turn",
        cost_estimate=pl.CostEstimate(flops=4 * 10**9, bytes_accessed=10**7, transcendentals=0),
    )(ids, at, field)
    place, gram = lax.optimization_barrier((at, gram))
    here = place[1]
    own_sum = sum_scatter(gram, here)
    own_masked, own_sum = lax.optimization_barrier((own_masked, own_sum))
    cross = pl.pallas_call(
        cross_kernel,
        out_shape=square,
        in_specs=[SMEM, VMEM, VMEM], out_specs=VMEM, compiler_params=limit(16), name="cross",
    )(at, own_masked, came)
    cross_sum = sum_scatter(cross, here)
    sums = sum_last(own_sum, cross_sum, place[0])
    rest = lax.ppermute(own, "st", swap)
    blocks = gather_all(sums, here)
    columns = pl.pallas_call(
        root_kernel,
        out_shape=struct((2 * states, states), bf16),
        in_specs=[SMEM, VMEM], out_specs=VMEM,
        scratch_shapes=[pltpu.VMEM((2 * states, 2 * states), f32), pltpu.VMEM((2, 2 * states, 2 * states), bf16)],
        compiler_params=limit(26), name="root",
    )(at, blocks)
    return rotate_call(at, columns, turned, came, rest)


def rotate_any(current, owned):
    states = current.shape[0]
    whole = lax.all_gather(current, "st", axis=0, tiled=True)
    rows = lax.dot_general(
        current * owned, whole, (((1,), (1,)), ((), ())), preferred_element_type=jnp.float32)
    gram = lax.all_gather(lax.psum(rows, "dom"), "st", axis=0, tiled=True)
    columns = lax.dynamic_slice_in_dim(inverse_root(gram), lax.axis_index("st") * states, states, 1)
    rotated = lax.dot_general(
        columns, whole, (((0,), (0,)), ((), ())), preferred_element_type=jnp.float32)
    return rotated.astype(jnp.bfloat16)


def body(start_states, stiffness, cell_scale, potential, connectivity, shared_nodes, filter_bounds):
    block_states, nodes = start_states.shape
    tiles = pl.cdiv(block_states, LANES)
    states = tiles * LANES
    if states != block_states:
        start_states = jnp.pad(start_states, ((0, states - block_states), (0, 0)))
    conn = connectivity.reshape(-1, LANES) * tiles
    ids = shared_nodes.reshape(-1) * tiles
    numbers = jnp.concatenate([cell_scale, filter_bounds])
    at = jnp.stack([lax.axis_index("st"), lax.axis_index("dom")])

    def exchange(low, high):
        return paired(low, "dom", 0), paired(high, "dom", 1)

    older = None
    current, total, low, high, pot, stiff = apply_call(
        0, (conn, ids, numbers, at), potential, stiffness, start_states)
    for step in range(DEGREE):
        came = exchange(low, high)
        last = step == DEGREE - 1
        following, *rest = settle_call(step, last, numbers, pot, current, total, older)
        if not last:
            older = current
            current, total, low, high = apply_call(
                step + 1, (conn, ids, numbers, at), pot, stiff, following, rest[0], *came)
            continue
    field, away = pl.pallas_call(
        send_kernel,
        out_shape=[struct(following.shape), struct((nodes // 2, states), jnp.bfloat16)],
        in_specs=[SMEM] * 3 + [VMEM] * 3,
        out_specs=[VMEM] * 2,
        scratch_shapes=[pltpu.VMEM((ids.shape[0] // 2 * tiles, LANES), jnp.float32)],
        input_output_aliases={3: 0},
        compiler_params=limit(26),
        name="send",
    )(ids, numbers, at, following, *came)
    devices = lax.axis_size("dom")
    if lax.axis_size("st") == 2 and states == block_states and devices & (devices - 1) == nodes % (4 * LANES):
        return rotate_pair(field, away, ids, at, states, nodes)
    current = field.reshape(nodes, states).T.astype(jnp.bfloat16)[:block_states]
    inside = (jnp.arange(nodes) < LN).astype(jnp.bfloat16)
    keep = jnp.where(lax.axis_index("dom") > 0, 0.0, 1.0).astype(jnp.bfloat16)
    owned = inside.at[shared_nodes[0, 0]].set(keep)[None, :]
    return rotate_any(current, owned)


def solution(mesh):
    placed = (P("st", "dom"), P(), P("dom"), P("dom"), P("dom", None), P("dom", None, None), P())
    return jax.shard_map(body, mesh=mesh, in_specs=placed, out_specs=P("st", "dom"), check_vma=False)
```

```python
import functools
import jax
import jax.numpy as jnp
from jax import lax
from jax.experimental import pallas as pl
from jax.experimental.pallas import tpu as pltpu
from jax.sharding import PartitionSpec as P


DEGREE = 3
NS_ITERS = 3
LN = 3480
LANES = 128
BATCH = 16
GROUP = 2
SPAN = 128
WIDTH = 256


def paired(x, axis, offset):
    devices = lax.axis_size(axis)
    firsts = range(offset, devices - 1, 2)
    pairs = [(i, i + 1) for i in firsts] + [(i + 1, i) for i in firsts]
    return lax.ppermute(x, axis, pairs)


def inverse_root(gram):
    frobenius = jnp.sqrt(jnp.sum(gram * gram) + 1e-06)
    iterate = gram / frobenius
    identity = jnp.eye(gram.shape[0], dtype=jnp.float32)
    inverse = identity
    for _ in range(NS_ITERS):
        factor = 1.5 * identity - 0.5 * jnp.dot(inverse, iterate, precision=lax.Precision.HIGHEST)
        iterate = jnp.dot(iterate, factor, precision=lax.Precision.HIGHEST)
        inverse = jnp.dot(factor, inverse, precision=lax.Precision.HIGHEST)
    return (inverse / jnp.sqrt(frobenius)).astype(jnp.bfloat16)


def batches(count, size, body):
    whole, rest = divmod(count, size)

    def step(g, carry):
        body(pl.multiple_of(g * size, size), size)
        return carry

    lax.fori_loop(0, whole, step, 0)
    if rest:
        body(whole * size, rest)


def add_faces(field, came, wide, ids, at, scale):
    count = ids.shape[0] // 2
    tiles = wide.shape[0] // count
    for slot in range(2):
        wide[...] = came[slot][...].astype(jnp.float32) * scale
        offset = side_of(slot, at) * count

        def add(base, size):
            first = offset + base
            rows = [pl.ds(ids[first + i], tiles) for i in range(size)]
            old = [field[row, :] for row in rows]
            new = [old[i] + wide[pl.ds((base + i) * tiles, tiles), :] for i in range(size)]
            for i in range(size):
                field[rows[i], :] = new[i]

        batches(count, BATCH, add)


def side_of(slot, at):
    odd = at[1] % 2
    return odd if slot else 1 - odd


def rounded(x):
    return x.astype(jnp.bfloat16).astype(jnp.float32)


def slope(bounds, times):
    return (2.0 * times) / jnp.full((1, LANES), bounds[bounds.shape[0] - 1] - bounds[bounds.shape[0] - 2], jnp.float32)


def apply_kernel(step, *refs):
    if step == 0:
        (conn, ids, scales, at, pot_row, stiff_in, start,
         field, total, below, above, pot, stiff, gathered, products, wide) = refs
    else:
        (conn, ids, scales, at, pot, stiff, _, _, came_low, came_high,
         field, total, below, above, gathered, products, wide) = refs
    dofs = stiff.shape[0]
    cells = conn.shape[0] * LANES // dofs
    count = ids.shape[0] // 2
    tiles = gathered.shape[0] // (GROUP * dofs)
    nodes = field.shape[0] // tiles
    if step == 0:
        width = 512
        pieces = nodes // width
        for k in range(pieces):
            spread = jnp.broadcast_to(pot_row[k * width:(k + 1) * width].reshape(1, width), (LANES, width)).T
            piece = start[:, k * width:(k + 1) * width].astype(jnp.float32)
            node = lax.broadcasted_iota(jnp.int32, piece.shape, 1) + k * width
            turned = jnp.where(node < LN, piece, 0.0).T
            for j in range(tiles):
                rows = pl.ds(k * width * tiles + j, width, tiles)
                field[rows, :] = turned[:, j * LANES:(j + 1) * LANES]
                pot[rows, :] = spread
                total[rows, :] = jnp.zeros_like(spread)
        stiff[...] = stiff_in[...].T
    else:
        add_faces(field, (came_low, came_high), wide, ids, at, slope(scales, min(step, 2)))

    lines = conn.shape[0] // cells * GROUP

    def gather(line, base):
        for i in range(BATCH):
            gathered[pl.ds((line % lines * LANES + base + i) * tiles, tiles), :] = field[
                pl.ds(conn[line, base + i], tiles), :]

    def gather_line(line):
        for base in range(0, LANES, BATCH):
            gather(line, base)

    def scatter_line(line, following):
        for base in range(0, LANES, BATCH):
            rows = [pl.ds(conn[line, base + i], tiles) for i in range(BATCH)]
            old = [total[row, :] for row in rows]
            first = (line % lines * LANES + base) * tiles
            new = [old[i] + products[pl.ds(first + i * tiles, tiles), :] for i in range(BATCH)]
            for i in range(BATCH):
                total[rows[i], :] = new[i]
            gather(following, base)

    def begin(line, carry):
        gather_line(line)
        return carry

    lax.fori_loop(0, lines, begin, 0)

    def some_cells(group, carry):
        values = jnp.concatenate(
            [gathered[pl.ds(c * dofs * tiles + j, dofs, tiles), :].astype(jnp.bfloat16)
             for c in range(GROUP) for j in range(tiles)], axis=1)
        result = jnp.dot(stiff[...], values, preferred_element_type=jnp.float32)
        for c in range(GROUP):
            scale = scales[group * GROUP + c]
            for j in range(tiles):
                at_lane = (c * tiles + j) * LANES
                products[pl.ds(c * dofs * tiles + j, dofs, tiles), :] = result[:, at_lane:at_lane + LANES] * scale
        following = jnp.minimum(group + 1, cells // GROUP - 1)

        def some(r, carried):
            scatter_line(group * lines + r, following * lines + r)
            return carried

        lax.fori_loop(0, lines, some, 0)
        return carry

    lax.fori_loop(0, cells // GROUP, some_cells, 0)

    for slot, faces in enumerate((below, above)):
        offset = side_of(slot, at) * count

        def take(base, size):
            first = offset + base
            for i in range(size):
                row = pl.ds(ids[first + i], tiles)
                wide[pl.ds((base + i) * tiles, tiles), :] = total[row, :] + pot[row, :] * rounded(field[row, :])

        batches(count, BATCH, take)
        faces[...] = wide[...].astype(faces.dtype)


def settle_kernel(step, last, *refs):
    if step == 0:
        bounds, pot, current, summed, out, total = refs
    else:
        bounds, pot, current, summed, older, out, *total = refs
        total = total[0] if total else None
    center = (bounds[bounds.shape[0] - 1] + bounds[bounds.shape[0] - 2]) * 0.5
    rate = slope(bounds, min(step + 1, 2))

    def some(g, carry):
        rows = pl.ds(pl.multiple_of(g * SPAN, SPAN), SPAN)
        value = rate * (summed[rows, :] + (pot[rows, :] - center) * rounded(current[rows, :]))
        if step:
            value = value - rounded(older[rows, :])
        out[rows, :] = value
        if not last:
            total[rows, :] = jnp.zeros_like(value)
        return carry

    lax.fori_loop(0, current.shape[0] // SPAN, some, 0)


def node_rows(field, start, width, tiles):
    return jnp.concatenate(
        [field[pl.ds(start * tiles + j, width, tiles), :] for j in range(tiles)], axis=1)


def send_kernel(ids, bounds, at, before, came_low, came_high, field, away, wide):
    count = ids.shape[0] // 2
    tiles = wide.shape[0] // count
    half = away.shape[0]
    add_faces(field, (came_low, came_high), wide, ids, at, slope(bounds, 2))
    start = (1 - at[0]) * half
    width = WIDTH
    for k in range(half // width):
        away[k * width:(k + 1) * width, :] = node_rows(
            field, start + k * width, width, tiles).astype(away.dtype)


def turn_kernel(ids, at, before, field, turned, own, own_masked, gram):
    count = ids.shape[0] // 2
    states, nodes = turned.shape
    tiles = states // LANES
    half = own.shape[0]
    start = pl.multiple_of(at[0] * half, LANES)
    width = WIDTH
    for k in range(half // width):
        own[k * width:(k + 1) * width, :] = node_rows(
            field, start + k * width, width, tiles).astype(own.dtype)
    for k in range(nodes // width):
        turned[:, k * width:(k + 1) * width] = node_rows(field, k * width, width, tiles).T.astype(turned.dtype)

    @pl.when(at[1] > 0)
    def _():
        def drop(base, size):
            for i in range(size):
                field[pl.ds(ids[base + i], tiles), :] = jnp.zeros((tiles, LANES), jnp.float32)

        batches(count, BATCH, drop)

    for k in range(half // width):
        own_masked[:, k * width:(k + 1) * width] = node_rows(
            field, start + k * width, width, tiles).T.astype(own_masked.dtype)
    total = jnp.zeros((states, states), jnp.float32)
    for k in range(nodes // width):
        total += jnp.dot(turned[:, k * width:(k + 1) * width],
                         node_rows(field, k * width, width, tiles).astype(turned.dtype),
                         preferred_element_type=jnp.float32)
    gram[...] = total


def cross_kernel(at, mine, came, out):
    value = jnp.dot(mine[...], came[...], preferred_element_type=jnp.float32)

    @pl.when(at[0] == 0)
    def _():
        out[...] = value

    @pl.when(at[0] != 0)
    def _():
        out[...] = value.T


def split(x):
    high = x.astype(jnp.bfloat16)
    return high, (x - high.astype(jnp.float32)).astype(jnp.bfloat16)


def product(a, b):
    def dot(x, y):
        return jnp.dot(x, y, preferred_element_type=jnp.float32)

    return dot(a[0], b[0]) + (dot(a[0], b[1]) + dot(a[1], b[0]))


def root_kernel(at, blocks, out, gram, held):
    size = blocks.shape[1]
    cross = blocks[2]
    gram[:size, :size] = blocks[0]
    gram[size:, size:] = blocks[1]
    gram[:size, size:] = cross
    gram[size:, :size] = cross.T
    whole = gram[...]
    scale = jnp.sqrt(jnp.sum(whole * whole, keepdims=True) + 1e-06)
    start = pl.multiple_of(at[0] * size, LANES)
    row = lax.broadcasted_iota(jnp.int32, whole.shape, 0)
    column = lax.broadcasted_iota(jnp.int32, whole.shape, 1)
    diagonal = jnp.where(row == column, 1.5, 0.0)
    iterate = whole / scale
    factor = diagonal - 0.5 * iterate
    inverse = None
    for sweep in range(1, NS_ITERS):
        pieces = split(factor)
        iterate = product(split(iterate), split(product(pieces, pieces)))
        factor = diagonal - 0.5 * iterate
        held[0], held[1] = pieces if inverse is None else inverse
        if sweep == NS_ITERS - 1:
            columns = held[0, :, pl.ds(start, size)], held[1, :, pl.ds(start, size)]
            result = product(split(factor), split(product(pieces, columns)))
        else:
            inverse = pieces if inverse is None else split(product(pieces, inverse))
    out[...] = (result / jnp.sqrt(scale)).astype(jnp.bfloat16)


def rotate_kernel(at, columns, turned, first, rest, out):
    states, nodes = out.shape
    half = nodes // 2
    own = columns[pl.ds(pl.multiple_of(at[0] * states, states), states), :]
    other = columns[pl.ds(pl.multiple_of((1 - at[0]) * states, states), states), :]

    def part_of(base, came):
        width = came.shape[0]
        base = pl.multiple_of(base, LANES)
        value = lax.dot_general(
            own, turned[:, pl.ds(base, width)], (((0,), (0,)), ((), ())), preferred_element_type=jnp.float32)
        value += lax.dot_general(
            other, came[...], (((0,), (1,)), ((), ())), preferred_element_type=jnp.float32)
        out[:, pl.ds(base, width)] = value.astype(out.dtype)

    part_of(at[0] * half, first)
    part_of((1 - at[0]) * half, rest)


def rotate_call(at, columns, turned, *came):
    return pl.pallas_call(
        rotate_kernel,
        out_shape=struct(turned.shape, jnp.bfloat16),
        in_specs=[SMEM] + [VMEM] * 4, out_specs=VMEM, compiler_params=limit(26), name="rotate",
    )(at, columns, turned, *came)


SMEM = pl.BlockSpec(memory_space=pltpu.SMEM)
VMEM = pl.BlockSpec(memory_space=pltpu.VMEM)


def limit(mib):
    return pltpu.CompilerParams(vmem_limit_bytes=mib * 1024 * 1024)


def struct(shape, dtype=jnp.float32):
    return jax.ShapeDtypeStruct(shape, dtype)


def apply_call(step, tables, pot, stiff, *fields):
    _, ids = tables[:2]
    dofs = stiff.shape[0]
    count = ids.shape[0] // 2
    f32, bf16 = jnp.float32, jnp.bfloat16
    if step == 0:
        tiles = fields[0].shape[0] // LANES
        rows = fields[0].shape[1] * tiles
    else:
        rows = pot.shape[0]
        tiles = fields[2].shape[0] // count
    face = struct((count * tiles, LANES), bf16)
    whole = struct((rows, LANES))
    out_shape = [whole, whole, face, face]
    if step == 0:
        out_shape += [whole, struct(stiff.shape, stiff.dtype)]
    scratch = [
        pltpu.VMEM((GROUP * dofs * tiles, LANES), f32),
        pltpu.VMEM((GROUP * dofs * tiles, LANES), f32),
        pltpu.VMEM((count * tiles, LANES), f32),
    ]
    specs = [VMEM] * (2 + len(fields))
    return pl.pallas_call(
        functools.partial(apply_kernel, step),
        out_shape=out_shape,
        in_specs=[SMEM] * 4 + specs,
        out_specs=[VMEM] * len(out_shape),
        scratch_shapes=scratch,
        input_output_aliases={6: 0, 7: 1} if step else {},
        compiler_params=limit(26),
        name="apply",
    )(*tables, pot, stiff, *fields)


def settle_call(step, last, bounds, pot, current, total, older=None):
    whole = struct(current.shape)
    fields = [current, total] + ([older] if step else [])
    aliases = {4: 0} if step else {}
    if not last:
        aliases[3] = 1
    return pl.pallas_call(
        functools.partial(settle_kernel, step, last),
        out_shape=[whole] if last else [whole, whole],
        in_specs=[SMEM] + [VMEM] * (1 + len(fields)),
        out_specs=[VMEM] * (1 if last else 2),
        input_output_aliases=aliases,
        compiler_params=limit(26),
        cost_estimate=pl.CostEstimate(flops=8 * 10**9, bytes_accessed=10**7, transcendentals=0),
        name="settle",
    )(bounds, pot, *fields)


def groups_of(devices):
    bits = devices.bit_length() - 1
    return [list(range(b, min(b + 2, bits))) if b else [0] for b in [0] + list(range(1, bits, 2))][:bits]


def plan(group):
    for m in range(1, 1 << len(group)):
        yield m, sum(((m >> i) & 1) << bit for i, bit in enumerate(group))


def code_of(group, here):
    return sum(((here >> bit) & 1) << i for i, bit in enumerate(group))


def sum_scatter(x, here):
    devices = lax.axis_size("dom")
    for group in groups_of(devices)[:-1]:
        size = x.shape[-2] >> len(group)
        code = code_of(group, here)
        came = [
            lax.ppermute(
                lax.dynamic_slice_in_dim(x, (code ^ m) * size, size, x.ndim - 2),
                "dom", [(i, i ^ mask) for i in range(devices)])
            for m, mask in plan(group)
        ]
        x = lax.dynamic_slice_in_dim(x, code * size, size, x.ndim - 2)
        for y in came:
            x = x + y
    return x


def sum_last(own, cross, part):
    devices = lax.axis_size("dom")
    both = jnp.stack([own, cross])
    sums = []
    for flip in range(2):
        total = None
        for m, mask in [(0, 0)] + list(plan(groups_of(devices)[-1])):
            piece = both
            if mask or flip:
                piece = lax.ppermute(both, ("dom", "st"), [(i, i ^ (2 * mask + flip)) for i in range(2 * devices)])
            total = piece if total is None else total + piece
        sums.append(total)
    mine, theirs = sums
    return jnp.stack([jnp.where(part == 0, mine[0], theirs[0]),
                      jnp.where(part == 0, theirs[0], mine[0]), mine[1] + theirs[1]])


def gather_all(x, here):
    devices = lax.axis_size("dom")
    for group in reversed(groups_of(devices)[:-1]):
        size = x.shape[-2]
        code = code_of(group, here)
        pieces = [(0, x)] + [
            (m, lax.ppermute(x, "dom", [(i, i ^ mask) for i in range(devices)])) for m, mask in plan(group)
        ]
        x = jnp.zeros(x.shape[:-2] + (size << len(group), x.shape[-1]), x.dtype)
        for m, piece in pieces:
            x = lax.dynamic_update_slice_in_dim(x, piece, (code ^ m) * size, x.ndim - 2)
    return x


def rotate_pair(field, away, ids, at, states, nodes):
    f32, bf16 = jnp.float32, jnp.bfloat16
    swap = [(0, 1), (1, 0)]
    half = nodes // 2
    square = struct((states, states))
    came = lax.ppermute(away, "st", swap)
    _, turned, own, own_masked, gram = pl.pallas_call(
        turn_kernel,
        out_shape=[struct(field.shape), struct((states, nodes), bf16),
                   struct((half, states), bf16),
                   struct((states, half), bf16), square],
        in_specs=[SMEM, SMEM, VMEM], out_specs=[VMEM] * 5,
        input_output_aliases={2: 0},
        compiler_params=limit(26), name="turn",
        cost_estimate=pl.CostEstimate(flops=4 * 10**9, bytes_accessed=10**7, transcendentals=0),
    )(ids, at, field)
    place, gram = lax.optimization_barrier((at, gram))
    here = place[1]
    own_sum = sum_scatter(gram, here)
    own_masked, own_sum = lax.optimization_barrier((own_masked, own_sum))
    cross = pl.pallas_call(
        cross_kernel,
        out_shape=square,
        in_specs=[SMEM, VMEM, VMEM], out_specs=VMEM, compiler_params=limit(16), name="cross",
    )(at, own_masked, came)
    cross_sum = sum_scatter(cross, here)
    sums = sum_last(own_sum, cross_sum, place[0])
    rest = lax.ppermute(own, "st", swap)
    blocks = gather_all(sums, here)
    columns = pl.pallas_call(
        root_kernel,
        out_shape=struct((2 * states, states), bf16),
        in_specs=[SMEM, VMEM], out_specs=VMEM,
        scratch_shapes=[pltpu.VMEM((2 * states, 2 * states), f32), pltpu.VMEM((2, 2 * states, 2 * states), bf16)],
        compiler_params=limit(26), name="root",
    )(at, blocks)
    return rotate_call(at, columns, turned, came, rest)


def rotate_any(current, owned):
    states = current.shape[0]
    whole = lax.all_gather(current, "st", axis=0, tiled=True)
    rows = lax.dot_general(
        current * owned, whole, (((1,), (1,)), ((), ())), preferred_element_type=jnp.float32)
    gram = lax.all_gather(lax.psum(rows, "dom"), "st", axis=0, tiled=True)
    columns = lax.dynamic_slice_in_dim(inverse_root(gram), lax.axis_index("st") * states, states, 1)
    rotated = lax.dot_general(
        columns, whole, (((0,), (0,)), ((), ())), preferred_element_type=jnp.float32)
    return rotated.astype(jnp.bfloat16)


def body(start_states, stiffness, cell_scale, potential, connectivity, shared_nodes, filter_bounds):
    block_states, nodes = start_states.shape
    tiles = pl.cdiv(block_states, LANES)
    states = tiles * LANES
    if states != block_states:
        start_states = jnp.pad(start_states, ((0, states - block_states), (0, 0)))
    conn = connectivity.reshape(-1, LANES) * tiles
    ids = shared_nodes.reshape(-1) * tiles
    numbers = jnp.concatenate([cell_scale, filter_bounds])
    at = jnp.stack([lax.axis_index("st"), lax.axis_index("dom")])

    def exchange(near, far):
        far = paired(far, "dom", 1)
        return paired(near, "dom", 0), far

    older = None
    current, total, low, high, pot, stiff = apply_call(
        0, (conn, ids, numbers, at), potential, stiffness, start_states)
    for step in range(DEGREE):
        came = exchange(low, high)
        last = step == DEGREE - 1
        following, *rest = settle_call(step, last, numbers, pot, current, total, older)
        if not last:
            older = current
            current, total, low, high = apply_call(
                step + 1, (conn, ids, numbers, at), pot, stiff, following, rest[0], *came)
            continue
    field, away = pl.pallas_call(
        send_kernel,
        out_shape=[struct(following.shape), struct((nodes // 2, states), jnp.bfloat16)],
        in_specs=[SMEM] * 3 + [VMEM] * 3,
        out_specs=[VMEM] * 2,
        scratch_shapes=[pltpu.VMEM((ids.shape[0] // 2 * tiles, LANES), jnp.float32)],
        input_output_aliases={3: 0},
        compiler_params=limit(26),
        name="send",
    )(ids, numbers, at, following, *came)
    devices = lax.axis_size("dom")
    if lax.axis_size("st") == 2 and states == block_states and devices & (devices - 1) == nodes % (4 * LANES):
        return rotate_pair(field, away, ids, at, states, nodes)
    current = field.reshape(nodes, states).T.astype(jnp.bfloat16)[:block_states]
    inside = (jnp.arange(nodes) < LN).astype(jnp.bfloat16)
    keep = jnp.where(lax.axis_index("dom") > 0, 0.0, 1.0).astype(jnp.bfloat16)
    owned = inside.at[shared_nodes[0, 0]].set(keep)[None, :]
    return rotate_any(current, owned)


def solution(mesh):
    placed = (P("st", "dom"), P(), P("dom"), P("dom"), P("dom", None), P("dom", None, None), P())
    return jax.shard_map(body, mesh=mesh, in_specs=placed, out_specs=P("st", "dom"), check_vma=False)
```

```python
import functools
import jax
import jax.numpy as jnp
from jax import lax
from jax.experimental import pallas as pl
from jax.experimental.pallas import tpu as pltpu
from jax.sharding import PartitionSpec as P


DEGREE = 3
NS_ITERS = 3
LN = 3480
LANES = 128
BATCH = 16
GROUP = 2
SPAN = 128
WIDTH = 256


def paired(x, axis, offset):
    devices = lax.axis_size(axis)
    firsts = range(offset, devices - 1, 2)
    pairs = [(i, i + 1) for i in firsts] + [(i + 1, i) for i in firsts]
    return lax.ppermute(x, axis, pairs)


def inverse_root(gram):
    frobenius = jnp.sqrt(jnp.sum(gram * gram) + 1e-06)
    iterate = gram / frobenius
    identity = jnp.eye(gram.shape[0], dtype=jnp.float32)
    inverse = identity
    for _ in range(NS_ITERS):
        factor = 1.5 * identity - 0.5 * jnp.dot(inverse, iterate, precision=lax.Precision.HIGHEST)
        iterate = jnp.dot(iterate, factor, precision=lax.Precision.HIGHEST)
        inverse = jnp.dot(factor, inverse, precision=lax.Precision.HIGHEST)
    return (inverse / jnp.sqrt(frobenius)).astype(jnp.bfloat16)


def batches(count, size, body):
    whole, rest = divmod(count, size)

    def step(g, carry):
        body(pl.multiple_of(g * size, size), size)
        return carry

    lax.fori_loop(0, whole, step, 0)
    if rest:
        body(whole * size, rest)


def add_faces(field, came, wide, ids, at, scale):
    count = ids.shape[0] // 2
    tiles = wide.shape[0] // count
    for slot in range(2):
        wide[...] = came[slot][...].astype(jnp.float32) * scale
        offset = side_of(slot, at) * count

        def add(base, size):
            first = offset + base
            rows = [pl.ds(ids[first + i], tiles) for i in range(size)]
            old = [field[row, :] for row in rows]
            new = [old[i] + wide[pl.ds((base + i) * tiles, tiles), :] for i in range(size)]
            for i in range(size):
                field[rows[i], :] = new[i]

        batches(count, BATCH, add)


def side_of(slot, at):
    odd = at[1] % 2
    return odd if slot else 1 - odd


def rounded(x):
    return x.astype(jnp.bfloat16).astype(jnp.float32)


def slope(bounds, times):
    return (2.0 * times) / jnp.full((1, LANES), bounds[bounds.shape[0] - 1] - bounds[bounds.shape[0] - 2], jnp.float32)


def apply_kernel(step, *refs):
    if step == 0:
        (conn, ids, scales, at, pot_row, stiff_in, start,
         field, total, below, above, pot, stiff, gathered, products, wide) = refs
    else:
        (conn, ids, scales, at, pot, stiff, _, _, came_low, came_high,
         field, total, below, above, gathered, products, wide) = refs
    dofs = stiff.shape[0]
    cells = conn.shape[0] * LANES // dofs
    count = ids.shape[0] // 2
    tiles = gathered.shape[0] // (GROUP * dofs)
    nodes = field.shape[0] // tiles
    if step == 0:
        width = 512
        pieces = nodes // width
        for k in range(pieces):
            spread = jnp.broadcast_to(pot_row[k * width:(k + 1) * width].reshape(1, width), (LANES, width)).T
            piece = start[:, k * width:(k + 1) * width].astype(jnp.float32)
            node = lax.broadcasted_iota(jnp.int32, piece.shape, 1) + k * width
            turned = jnp.where(node < LN, piece, 0.0).T
            for j in range(tiles):
                rows = pl.ds(k * width * tiles + j, width, tiles)
                field[rows, :] = turned[:, j * LANES:(j + 1) * LANES]
                pot[rows, :] = spread
                total[rows, :] = jnp.zeros_like(spread)
        stiff[...] = stiff_in[...].T
    else:
        add_faces(field, (came_low, came_high), wide, ids, at, slope(scales, min(step, 2)))

    lines = conn.shape[0] // cells * GROUP

    def gather(line, base):
        for i in range(BATCH):
            gathered[pl.ds((line % lines * LANES + base + i) * tiles, tiles), :] = field[
                pl.ds(conn[line, base + i], tiles), :]

    def gather_line(line):
        for base in range(0, LANES, BATCH):
            gather(line, base)

    def scatter_line(line, following):
        for base in range(0, LANES, BATCH):
            rows = [pl.ds(conn[line, base + i], tiles) for i in range(BATCH)]
            old = [total[row, :] for row in rows]
            first = (line % lines * LANES + base) * tiles
            new = [old[i] + products[pl.ds(first + i * tiles, tiles), :] for i in range(BATCH)]
            for i in range(BATCH):
                total[rows[i], :] = new[i]
            gather(following, base)

    def begin(line, carry):
        gather_line(line)
        return carry

    lax.fori_loop(0, lines, begin, 0)

    def some_cells(group, carry):
        values = jnp.concatenate(
            [gathered[pl.ds(c * dofs * tiles + j, dofs, tiles), :].astype(jnp.bfloat16)
             for c in range(GROUP) for j in range(tiles)], axis=1)
        result = jnp.dot(stiff[...], values, preferred_element_type=jnp.float32)
        for c in range(GROUP):
            scale = scales[group * GROUP + c]
            for j in range(tiles):
                at_lane = (c * tiles + j) * LANES
                products[pl.ds(c * dofs * tiles + j, dofs, tiles), :] = result[:, at_lane:at_lane + LANES] * scale
        following = jnp.minimum(group + 1, cells // GROUP - 1)

        def some(r, carried):
            scatter_line(group * lines + r, following * lines + r)
            return carried

        lax.fori_loop(0, lines, some, 0)
        return carry

    lax.fori_loop(0, cells // GROUP, some_cells, 0)

    for slot, faces in enumerate((below, above)):
        offset = side_of(slot, at) * count

        def take(base, size):
            first = offset + base
            for i in range(size):
                row = pl.ds(ids[first + i], tiles)
                wide[pl.ds((base + i) * tiles, tiles), :] = total[row, :] + pot[row, :] * rounded(field[row, :])

        batches(count, BATCH, take)
        faces[...] = wide[...].astype(faces.dtype)


def settle_kernel(step, last, *refs):
    if step == 0:
        bounds, pot, current, summed, out, total = refs
    else:
        bounds, pot, current, summed, older, out, *total = refs
        total = total[0] if total else None
    center = (bounds[bounds.shape[0] - 1] + bounds[bounds.shape[0] - 2]) * 0.5
    rate = slope(bounds, min(step + 1, 2))

    def some(g, carry):
        rows = pl.ds(pl.multiple_of(g * SPAN, SPAN), SPAN)
        value = rate * (summed[rows, :] + (pot[rows, :] - center) * rounded(current[rows, :]))
        if step:
            value = value - rounded(older[rows, :])
        out[rows, :] = value
        if not last:
            total[rows, :] = jnp.zeros_like(value)
        return carry

    lax.fori_loop(0, current.shape[0] // SPAN, some, 0)


def node_rows(field, start, width, tiles):
    return jnp.concatenate(
        [field[pl.ds(start * tiles + j, width, tiles), :] for j in range(tiles)], axis=1)


def send_kernel(ids, bounds, at, before, came_low, came_high, field, away, wide):
    count = ids.shape[0] // 2
    tiles = wide.shape[0] // count
    half = away.shape[0]
    add_faces(field, (came_low, came_high), wide, ids, at, slope(bounds, 2))
    start = (1 - at[0]) * half
    width = WIDTH
    for k in range(half // width):
        away[k * width:(k + 1) * width, :] = node_rows(
            field, start + k * width, width, tiles).astype(away.dtype)


def turn_kernel(ids, at, before, field, turned, own, own_masked, gram):
    count = ids.shape[0] // 2
    states, nodes = turned.shape
    tiles = states // LANES
    half = own.shape[0]
    start = pl.multiple_of(at[0] * half, LANES)
    width = WIDTH
    for k in range(half // width):
        own[k * width:(k + 1) * width, :] = node_rows(
            field, start + k * width, width, tiles).astype(own.dtype)
    for k in range(nodes // width):
        turned[:, k * width:(k + 1) * width] = node_rows(field, k * width, width, tiles).T.astype(turned.dtype)

    @pl.when(at[1] > 0)
    def _():
        def drop(base, size):
            for i in range(size):
                field[pl.ds(ids[base + i], tiles), :] = jnp.zeros((tiles, LANES), jnp.float32)

        batches(count, BATCH, drop)

    for k in range(half // width):
        own_masked[:, k * width:(k + 1) * width] = node_rows(
            field, start + k * width, width, tiles).T.astype(own_masked.dtype)
    total = jnp.zeros((states, states), jnp.float32)
    for k in range(nodes // width):
        total += jnp.dot(turned[:, k * width:(k + 1) * width],
                         node_rows(field, k * width, width, tiles).astype(turned.dtype),
                         preferred_element_type=jnp.float32)
    gram[...] = total


def cross_kernel(at, mine, came, out):
    value = jnp.dot(mine[...], came[...], preferred_element_type=jnp.float32)

    @pl.when(at[0] == 0)
    def _():
        out[...] = value

    @pl.when(at[0] != 0)
    def _():
        out[...] = value.T


def split(x):
    high = x.astype(jnp.bfloat16)
    return high, (x - high.astype(jnp.float32)).astype(jnp.bfloat16)


def product(a, b):
    def dot(x, y):
        return jnp.dot(x, y, preferred_element_type=jnp.float32)

    return dot(a[0], b[0]) + (dot(a[0], b[1]) + dot(a[1], b[0]))


def root_kernel(at, blocks, out, gram, held):
    size = blocks.shape[1]
    cross = blocks[2]
    gram[:size, :size] = blocks[0]
    gram[size:, size:] = blocks[1]
    gram[:size, size:] = cross
    gram[size:, :size] = cross.T
    whole = gram[...]
    scale = jnp.sqrt(jnp.sum(whole * whole, keepdims=True) + 1e-06)
    start = pl.multiple_of(at[0] * size, LANES)
    row = lax.broadcasted_iota(jnp.int32, whole.shape, 0)
    column = lax.broadcasted_iota(jnp.int32, whole.shape, 1)
    diagonal = jnp.where(row == column, 1.5, 0.0)
    iterate = whole / scale
    factor = diagonal - 0.5 * iterate
    inverse = None
    for sweep in range(1, NS_ITERS):
        pieces = split(factor)
        iterate = product(split(iterate), split(product(pieces, pieces)))
        factor = diagonal - 0.5 * iterate
        held[0], held[1] = pieces if inverse is None else inverse
        if sweep == NS_ITERS - 1:
            columns = held[0, :, pl.ds(start, size)], held[1, :, pl.ds(start, size)]
            result = product(split(factor), split(product(pieces, columns)))
        else:
            inverse = pieces if inverse is None else split(product(pieces, inverse))
    out[...] = (result / jnp.sqrt(scale)).astype(jnp.bfloat16)


def rotate_kernel(at, columns, turned, first, rest, out):
    states, nodes = out.shape
    half = nodes // 2
    own = columns[pl.ds(pl.multiple_of(at[0] * states, states), states), :]
    other = columns[pl.ds(pl.multiple_of((1 - at[0]) * states, states), states), :]

    def part_of(base, came):
        width = came.shape[0]
        base = pl.multiple_of(base, LANES)
        value = lax.dot_general(
            own, turned[:, pl.ds(base, width)], (((0,), (0,)), ((), ())), preferred_element_type=jnp.float32)
        value += lax.dot_general(
            other, came[...], (((0,), (1,)), ((), ())), preferred_element_type=jnp.float32)
        out[:, pl.ds(base, width)] = value.astype(out.dtype)

    part_of(at[0] * half, first)
    part_of((1 - at[0]) * half, rest)


def rotate_call(at, columns, turned, *came):
    return pl.pallas_call(
        rotate_kernel,
        out_shape=struct(turned.shape, jnp.bfloat16),
        in_specs=[SMEM] + [VMEM] * 4, out_specs=VMEM, compiler_params=limit(26), name="rotate",
    )(at, columns, turned, *came)


SMEM = pl.BlockSpec(memory_space=pltpu.SMEM)
VMEM = pl.BlockSpec(memory_space=pltpu.VMEM)


def limit(mib):
    return pltpu.CompilerParams(vmem_limit_bytes=mib * 1024 * 1024)


def struct(shape, dtype=jnp.float32):
    return jax.ShapeDtypeStruct(shape, dtype)


def apply_call(step, tables, pot, stiff, *fields):
    _, ids = tables[:2]
    dofs = stiff.shape[0]
    count = ids.shape[0] // 2
    f32, bf16 = jnp.float32, jnp.bfloat16
    if step == 0:
        tiles = fields[0].shape[0] // LANES
        rows = fields[0].shape[1] * tiles
    else:
        rows = pot.shape[0]
        tiles = fields[2].shape[0] // count
    face = struct((count * tiles, LANES), bf16)
    whole = struct((rows, LANES))
    out_shape = [whole, whole, face, face]
    if step == 0:
        out_shape += [whole, struct(stiff.shape, stiff.dtype)]
    scratch = [
        pltpu.VMEM((GROUP * dofs * tiles, LANES), f32),
        pltpu.VMEM((GROUP * dofs * tiles, LANES), f32),
        pltpu.VMEM((count * tiles, LANES), f32),
    ]
    specs = [VMEM] * (2 + len(fields))
    return pl.pallas_call(
        functools.partial(apply_kernel, step),
        out_shape=out_shape,
        in_specs=[SMEM] * 4 + specs,
        out_specs=[VMEM] * len(out_shape),
        scratch_shapes=scratch,
        input_output_aliases={6: 0, 7: 1} if step else {},
        compiler_params=limit(26),
        name="apply",
    )(*tables, pot, stiff, *fields)


def settle_call(step, last, bounds, pot, current, total, older=None):
    whole = struct(current.shape)
    fields = [current, total] + ([older] if step else [])
    aliases = {4: 0} if step else {}
    if not last:
        aliases[3] = 1
    return pl.pallas_call(
        functools.partial(settle_kernel, step, last),
        out_shape=[whole] if last else [whole, whole],
        in_specs=[SMEM] + [VMEM] * (1 + len(fields)),
        out_specs=[VMEM] * (1 if last else 2),
        input_output_aliases=aliases,
        compiler_params=limit(26),
        cost_estimate=pl.CostEstimate(flops=8 * 10**9, bytes_accessed=10**7, transcendentals=0),
        name="settle",
    )(bounds, pot, *fields)


def groups_of(devices):
    bits = devices.bit_length() - 1
    return [list(range(b, min(b + 2, bits))) if b else [0] for b in [0] + list(range(1, bits, 2))][:bits]


def hop(x, pairs):
    return lax.ppermute(x, "dom", pairs)


def plan(group):
    for m in range(1, 1 << len(group)):
        yield m, sum(((m >> i) & 1) << bit for i, bit in enumerate(group))


def code_of(group, here):
    return sum(((here >> bit) & 1) << i for i, bit in enumerate(group))


def sum_scatter(x, here):
    devices = lax.axis_size("dom")
    for group in groups_of(devices)[:-1]:
        size = x.shape[-2] >> len(group)
        code = code_of(group, here)
        came = [
            hop(lax.dynamic_slice_in_dim(x, (code ^ m) * size, size, x.ndim - 2),
                [(i, i ^ mask) for i in range(devices)])
            for m, mask in plan(group)
        ]
        x = lax.dynamic_slice_in_dim(x, code * size, size, x.ndim - 2)
        for y in came:
            x = x + y
    return x


def sum_last(own, cross, part):
    devices = lax.axis_size("dom")
    both = jnp.stack([own, cross])
    sums = []
    for flip in range(2):
        total = None
        for m, mask in [(0, 0)] + list(plan(groups_of(devices)[-1])):
            piece = both
            if mask or flip:
                piece = lax.ppermute(both, ("dom", "st"), [(i, i ^ (2 * mask + flip)) for i in range(2 * devices)])
            total = piece if total is None else total + piece
        sums.append(total)
    mine, theirs = sums
    return jnp.stack([jnp.where(part == 0, mine[0], theirs[0]),
                      jnp.where(part == 0, theirs[0], mine[0]), mine[1] + theirs[1]])


def gather_all(x, here):
    devices = lax.axis_size("dom")
    for group in reversed(groups_of(devices)[:-1]):
        size = x.shape[-2]
        code = code_of(group, here)
        pieces = [(0, x)] + [(m, hop(x, [(i, i ^ mask) for i in range(devices)])) for m, mask in plan(group)]
        x = jnp.zeros(x.shape[:-2] + (size << len(group), x.shape[-1]), x.dtype)
        for m, piece in pieces:
            x = lax.dynamic_update_slice_in_dim(x, piece, (code ^ m) * size, x.ndim - 2)
    return x


def rotate_pair(field, away, ids, at, states, nodes):
    f32, bf16 = jnp.float32, jnp.bfloat16
    swap = [(0, 1), (1, 0)]
    half = nodes // 2
    square = struct((states, states))
    came = lax.ppermute(away, "st", swap)
    _, turned, own, own_masked, gram = pl.pallas_call(
        turn_kernel,
        out_shape=[struct(field.shape), struct((states, nodes), bf16),
                   struct((half, states), bf16),
                   struct((states, half), bf16), square],
        in_specs=[SMEM, SMEM, VMEM], out_specs=[VMEM] * 5,
        input_output_aliases={2: 0},
        compiler_params=limit(26), name="turn",
        cost_estimate=pl.CostEstimate(flops=4 * 10**9, bytes_accessed=10**7, transcendentals=0),
    )(ids, at, field)
    place, gram = lax.optimization_barrier((at, gram))
    here = place[1]
    own_sum = sum_scatter(gram, here)
    own_masked, own_sum = lax.optimization_barrier((own_masked, own_sum))
    cross = pl.pallas_call(
        cross_kernel,
        out_shape=square,
        in_specs=[SMEM, VMEM, VMEM], out_specs=VMEM, compiler_params=limit(16), name="cross",
    )(at, own_masked, came)
    cross_sum = sum_scatter(cross, here)
    sums = sum_last(own_sum, cross_sum, place[0])
    rest = lax.ppermute(own, "st", swap)
    blocks = gather_all(sums, here)
    columns = pl.pallas_call(
        root_kernel,
        out_shape=struct((2 * states, states), bf16),
        in_specs=[SMEM, VMEM], out_specs=VMEM,
        scratch_shapes=[pltpu.VMEM((2 * states, 2 * states), f32), pltpu.VMEM((2, 2 * states, 2 * states), bf16)],
        compiler_params=limit(26), name="root",
    )(at, blocks)
    return rotate_call(at, columns, turned, came, rest)


def rotate_any(current, owned):
    states = current.shape[0]
    whole = lax.all_gather(current, "st", axis=0, tiled=True)
    rows = lax.dot_general(
        current * owned, whole, (((1,), (1,)), ((), ())), preferred_element_type=jnp.float32)
    gram = lax.all_gather(lax.psum(rows, "dom"), "st", axis=0, tiled=True)
    columns = lax.dynamic_slice_in_dim(inverse_root(gram), lax.axis_index("st") * states, states, 1)
    rotated = lax.dot_general(
        columns, whole, (((0,), (0,)), ((), ())), preferred_element_type=jnp.float32)
    return rotated.astype(jnp.bfloat16)


def body(start_states, stiffness, cell_scale, potential, connectivity, shared_nodes, filter_bounds):
    block_states, nodes = start_states.shape
    tiles = pl.cdiv(block_states, LANES)
    states = tiles * LANES
    if states != block_states:
        start_states = jnp.pad(start_states, ((0, states - block_states), (0, 0)))
    conn = connectivity.reshape(-1, LANES) * tiles
    ids = shared_nodes.reshape(-1) * tiles
    numbers = jnp.concatenate([cell_scale, filter_bounds])
    at = jnp.stack([lax.axis_index("st"), lax.axis_index("dom")])

    def exchange(near, far):
        far = paired(far, "dom", 1)
        return paired(near, "dom", 0), far

    older = None
    current, total, low, high, pot, stiff = apply_call(
        0, (conn, ids, numbers, at), potential, stiffness, start_states)
    for step in range(DEGREE):
        came = exchange(low, high)
        last = step == DEGREE - 1
        following, *rest = settle_call(step, last, numbers, pot, current, total, older)
        if not last:
            older = current
            current, total, low, high = apply_call(
                step + 1, (conn, ids, numbers, at), pot, stiff, following, rest[0], *came)
            continue
    field, away = pl.pallas_call(
        send_kernel,
        out_shape=[struct(following.shape), struct((nodes // 2, states), jnp.bfloat16)],
        in_specs=[SMEM] * 3 + [VMEM] * 3,
        out_specs=[VMEM] * 2,
        scratch_shapes=[pltpu.VMEM((ids.shape[0] // 2 * tiles, LANES), jnp.float32)],
        input_output_aliases={3: 0},
        compiler_params=limit(26),
        name="send",
    )(ids, numbers, at, following, *came)
    devices = lax.axis_size("dom")
    if lax.axis_size("st") == 2 and states == block_states and devices & (devices - 1) == nodes % (4 * LANES):
        return rotate_pair(field, away, ids, at, states, nodes)
    current = field.reshape(nodes, states).T.astype(jnp.bfloat16)[:block_states]
    inside = (jnp.arange(nodes) < LN).astype(jnp.bfloat16)
    keep = jnp.where(lax.axis_index("dom") > 0, 0.0, 1.0).astype(jnp.bfloat16)
    owned = inside.at[shared_nodes[0, 0]].set(keep)[None, :]
    return rotate_any(current, owned)


def solution(mesh):
    placed = (P("st", "dom"), P(), P("dom"), P("dom"), P("dom", None), P("dom", None, None), P())
    return jax.shard_map(body, mesh=mesh, in_specs=placed, out_specs=P("st", "dom"), check_vma=False)
```
